256 devices in a mesh: row: 16 (over z, core), col: 16 (over y, x).
Axes of the slice: x: 4, y: 4, z: 8, core: 2. Of those that a mesh axis runs over, the one named last changes fastest.
Arguments:
- velocity: float32 [1, 3, 128, 256, 256], P(None, None, 'row', 'col'), may hold values from -6 to 6
- tendency: float32 [1, 3, 128, 256, 256], P(None, None, 'row', 'col'), may hold values from -6 to 6
- step_size: float32 [1], replicated, may hold values from 0.1 to 0.6
- lift_weight: float32 [32, 3], replicated, may hold values from -3.5 to 3.5
- lift_bias: float32 [32], replicated, may hold values from -3 to 3
- spectral_weight: bfloat16 [2, 32, 32, 32, 1024], P(None, 'row', 'col'), may hold values from -6 to 6
- local_weight: float32 [32, 32], replicated, may hold values from -1 to 1
- local_bias: float32 [32], replicated, may hold values from -3 to 3
Outputs:
- features: bfloat16 [1, 32, 128, 256, 256], P(None, None, 'row', 'col')
The draws below stay inside these ranges and needn't reach their ends.
All inputs are finite; a program needn't handle non-finite values.
Results may differ from the reference program's by a relative error of at most 0.001.
Values sent between devices are 32-bit elements; how exact they have to be, the bound alone decides.
No kernel may reach another device: no remote copies, remote signals or barrier semaphores. Data moves between devices by JAX's collectives and lax.ppermute only.
A program may use at most 64 MiB of HBM per device.

```python
import math
import jax
import jax.numpy as jnp
from jax import lax

CHANNELS = 32
KX = 32
KY = 32
KZ = 32
NZ = 256
SAMPLES = 1
NX = 128
NY = 256


def block_levels(key, dims, shards, low, high):
    factor_of, own = 1.0, jax.random.fold_in(key, 6)
    for position, shards_of in shards:
        heights = jnp.exp(jax.random.uniform(jax.random.fold_in(own, position), (shards_of,), jnp.float32, low / len(shards), high / len(shards)))
        factor_of = factor_of * jnp.repeat(heights, dims[position] // shards_of).reshape([-1 if axis == position else 1 for axis in range(len(dims))])
    return factor_of


def centred(key, dims, scale, reach, pieces=(), kind=jnp.bfloat16):
    gain = block_levels(key, dims, pieces, -0.22, 0.18) if pieces else 1.0
    entries = jax.random.normal(key, dims, jnp.float32) * scale * gain
    return jnp.minimum(jnp.maximum(entries, -reach), reach).astype(kind)


def setup_inputs(seed: int = 0) -> dict:
    arg_keys = jax.random.split(jax.random.key(seed), 9)
    velocity = centred(arg_keys[0], (SAMPLES, 3, NX, NY, NZ), 1.0, 6.0, ((2, 16), (3, 16)), jnp.float32)
    tendency = centred(arg_keys[1], (SAMPLES, 3, NX, NY, NZ), 1.0, 6.0, ((2, 16), (3, 16)), jnp.float32)
    step_size = jnp.clip(jnp.exp(jax.random.uniform(arg_keys[2], (SAMPLES,), jnp.float32, math.log(0.1), math.log(0.6))), 0.1, 0.6)
    lift_weight = centred(arg_keys[3], (CHANNELS, 3), 3 ** -0.5, 3.5, (), jnp.float32)
    lift_bias = centred(arg_keys[4], (CHANNELS,), 0.5, 3.0, (), jnp.float32)
    spectral_weight = centred(arg_keys[5], (2, KY, KZ, KX, CHANNELS * CHANNELS), 1.0, 6.0, ((1, 16), (2, 16)))
    local_weight = centred(arg_keys[6], (CHANNELS, CHANNELS), CHANNELS ** -0.5, 1.0, (), jnp.float32)
    local_bias = centred(arg_keys[7], (CHANNELS,), 0.5, 3.0, (), jnp.float32)
    return dict(velocity=velocity, tendency=tendency, step_size=step_size, lift_weight=lift_weight, lift_bias=lift_bias, spectral_weight=spectral_weight, local_weight=local_weight, local_bias=local_bias)


def positions(count, length):
    index = jnp.arange(count, dtype=jnp.int32)
    return jnp.where(index < count // 2, index, length - count + index).astype(jnp.int32)


def reference(velocity, tendency, step_size, lift_weight, lift_bias, spectral_weight, local_weight, local_bias):
    highest = lax.Precision.HIGHEST
    x_pos = positions(KX, NX)
    y_pos = positions(KY, NY)
    z_pos = jnp.arange(KZ, dtype=jnp.int32)
    volume = NX * NY * NZ
    weights = spectral_weight.astype(jnp.float32).reshape(2, KY, KZ, KX, CHANNELS, CHANNELS)
    complex_weights = weights[0] + 1j * weights[1]
    combined = jnp.dot(local_weight, lift_weight, precision=highest)
    offset = jnp.dot(local_weight, lift_bias, precision=highest) + local_bias
    results = []
    for sample in range(SAMPLES):
        advanced = velocity[sample] + step_size[sample] * tendency[sample]

        def forward(channel):
            lifted = (lift_weight[channel, 0] * advanced[0] + lift_weight[channel, 1] * advanced[1]
                      + lift_weight[channel, 2] * advanced[2] + lift_bias[channel])
            spectrum = jnp.fft.rfftn(lifted)
            kept = spectrum[x_pos][:, y_pos][:, :, :KZ]
            return kept / volume

        coeffs = lax.map(forward, jnp.arange(CHANNELS, dtype=jnp.int32))
        mixed = jnp.einsum("egaoi,iaeg->oaeg", complex_weights, coeffs, precision=highest)

        def inverse(channel):
            full = jnp.zeros((NX, NY, NZ // 2 + 1), mixed.dtype)
            full = full.at[x_pos[:, None, None], y_pos[None, :, None], z_pos[None, None, :]].set(mixed[channel])
            spectral = jnp.fft.irfftn(full, s=(NX, NY, NZ)) * volume
            local = (combined[channel, 0] * advanced[0] + combined[channel, 1] * advanced[1]
                     + combined[channel, 2] * advanced[2] + offset[channel])
            return jax.nn.gelu(spectral + local).astype(jnp.bfloat16)

        results.append(lax.map(inverse, jnp.arange(CHANNELS, dtype=jnp.int32)))
    return jnp.stack(results, 0)
```

```python
import math

import jax
import jax.numpy as jnp
import numpy as np
from jax import lax
from jax.experimental import pallas as pl
from jax.experimental.pallas import tpu as pltpu
from jax.sharding import PartitionSpec as P

NX = 128
NY = 256
NZ = 256
KX = 32
KY = 32
KZ = 32
CH = 32
ROWS = 16
COLS = 16
F32 = jnp.float32
BF16 = jnp.bfloat16


def waves(count):
    index = np.arange(count)
    return np.where(index < count // 2, index, index - count)


def pair(table):
    high = table.astype(np.float32).astype(BF16)
    low = (table - high.astype(np.float64)).astype(np.float32).astype(BF16)
    return high, low


def z_forward():
    angle = 2 * math.pi * ((np.arange(KZ)[:, None] * np.arange(NZ)[None]) % NZ) / NZ
    high, low = pair(np.concatenate([np.cos(angle), -np.sin(angle)], 0))
    return np.concatenate([high, low], 0)


def y_forward():
    angle = 2 * math.pi * ((waves(KY)[:, None] * np.arange(16)[None]) % NY) / NY
    table = np.zeros((8, 16, 2, KY, 8))
    for x in range(8):
        table[x, :, 0, :, x] = np.cos(angle).T
        table[x, :, 1, :, x] = np.sin(angle).T
    high, low = pair(table.reshape(128, 512))
    return np.concatenate([high, high, low], 0)


def y_phase():
    angle = 2 * math.pi * ((waves(KY)[None] * 16 * np.arange(COLS)[:, None]) % NY) / NY
    scale = 1.0 / (NX * NY * NZ)
    table = np.stack([np.cos(angle), np.sin(angle)], 1) * scale
    return np.repeat(table, 8, axis=2).astype(np.float32)


def x_forward():
    angle = 2 * math.pi * ((waves(KX)[None] * np.arange(8)[:, None]) % NX) / NX
    table = np.zeros((4, 2, 2, 8, 2, 3, 2, 2, KX))
    cosine, sine = np.cos(angle), np.sin(angle)
    for c in range(3):
        for e in range(2):
            for d in range(2):
                table[c, 0, e, :, 0, c, e, d] = cosine
                table[c, 1, e, :, 0, c, e, d] = sine
                table[c, 1, e, :, 1, c, e, d] = cosine
                table[c, 0, e, :, 1, c, e, d] = -sine
    high, low = pair(table.reshape(128, 768))
    return np.concatenate([high, high, low], 0)


def x_phase():
    angle = 2 * math.pi * ((waves(KX)[None] * 8 * np.arange(ROWS)[:, None]) % NX) / NX
    table = np.stack([np.cos(angle), np.sin(angle)], 1)
    return np.tile(table, (1, 1, 4)).astype(np.float32)


def x_inverse():
    points = np.arange(NX).reshape(ROWS, 8)
    angle = 2 * math.pi * ((points[:, :, None] * waves(KX)) % NX) / NX
    table = np.zeros((ROWS, 2, 8, 2, KX))
    table[:, 0, :, 0] = np.cos(angle)
    table[:, 0, :, 1] = -np.sin(angle)
    table[:, 1, :, 0] = np.sin(angle)
    table[:, 1, :, 1] = np.cos(angle)
    high, low = pair(table.reshape(256, 64))
    return np.concatenate([high, high, low, low], 1)


def y_inverse():
    angle = 2 * math.pi * ((waves(KY)[:, None] * np.arange(NY)[None]) % NY) / NY
    angle = angle.reshape(ROWS, 2, NY).transpose(1, 0, 2)
    table = np.zeros((2, ROWS, 2, 2, NY))
    table[:, :, 0, 0] = np.cos(angle)
    table[:, :, 1, 0] = -np.sin(angle)
    table[:, :, 0, 1] = np.sin(angle)
    table[:, :, 1, 1] = np.cos(angle)
    high, low = pair(table.reshape(64, 512))
    return np.concatenate([high, high, low, low], 0)


def z_inverse():
    angle = 2 * math.pi * ((np.arange(KZ)[:, None] * np.arange(NZ)[None]) % NZ) / NZ
    double = np.where(np.arange(KZ) == 0, 1.0, 2.0)[:, None]
    angle = angle.reshape(COLS, 2, NZ)
    double = double.reshape(COLS, 2, 1)
    table = np.stack([double * np.cos(angle), -double * np.sin(angle)], 1)
    high, low = pair(table.reshape(64, NZ))
    return np.concatenate([high, high, low, low], 0)


def dot(a, b):
    return jnp.dot(a, b, preferred_element_type=F32)


def dot_t(a, b):
    return lax.dot_general(a, b, (((1,), (1,)), ((), ())), preferred_element_type=F32)


def split(value):
    high = value.astype(BF16)
    low = (value - high.astype(F32)).astype(BF16)
    return high, low


def exchange(arrays, axis, unit):
    arrays = list(arrays)
    length = arrays[0].shape[axis]
    place = lax.broadcasted_iota(jnp.int32, arrays[0].shape, axis)
    bit = 1
    while bit < len(arrays):
        shift = bit * unit
        keep = (place & shift) == 0
        for i in range(len(arrays)):
            if i & bit == 0:
                a, b = arrays[i], arrays[i | bit]
                arrays[i] = jnp.where(keep, a, pltpu.roll(b, shift, axis))
                arrays[i | bit] = jnp.where(keep, pltpu.roll(a, length - shift, axis), b)
        bit *= 2
    return arrays


def forward_kernel(place, step, velocity, tendency, z_table, y_table, phase, advanced, out):
    value = velocity[...] + step[0] * tendency[...]
    advanced[...] = value
    high, low = split(value)
    first = dot_t(z_table[...], high)
    modes = first[:64] + first[64:] + dot_t(z_table[0:64, :], low)
    modes = jnp.concatenate([modes[:, 128 * c : 128 * c + 128] for c in range(3)], 0)
    high, low = split(modes)
    table = y_table[...]
    sums = dot(jnp.concatenate([high, low], 1), table[:256]) + dot(high, table[256:])
    turn = phase[place[1]]
    cosine, sine = turn[0:1], turn[1:2]
    parts = []
    for c in range(3):
        real = sums[64 * c : 64 * c + 32]
        imag = sums[64 * c + 32 : 64 * c + 64]
        re = real[:, :256] + imag[:, 256:]
        im = imag[:, :256] - real[:, 256:]
        parts.append(re * cosine + im * sine)
        parts.append(im * cosine - re * sine)
    zero = jnp.zeros((32, 128), F32)
    for half in range(2):
        lanes = [p[:, 128 * half : 128 * half + 128] for p in parts] + [zero, zero]
        for g, block in enumerate(exchange(lanes, 1, 16)):
            out[8 * half + g] = block


def weight_kernel(weights, lift, out):
    row = lax.broadcasted_iota(jnp.int32, (32, 1024), 0)
    lane = lax.broadcasted_iota(jnp.int32, (32, 1024), 1)
    same = row == lane // 32
    maps = jnp.concatenate([jnp.where(same, lift[j : j + 1, :], 0.0) for j in range(4)], 0)
    high, rest = split(maps)
    rest_f = maps - high.astype(F32)
    mid = rest_f.astype(BF16)
    low = (rest_f - mid.astype(F32)).astype(BF16)
    w = weights[...]
    out[...] = dot_t(high, w) + dot_t(mid, w) + dot_t(low, w)


def mix_kernel(place, arrived, w_eff, x_table, phase, back_table, out):
    sums = []
    for r in range(ROWS):
        block = arrived[r]
        total = (block[0:8] + block[8:16]) + (block[16:24] + block[24:32])
        total = total + pltpu.roll(total, 4, 0)
        total = total + pltpu.roll(total, 2, 0)
        sums.append(total)
    high, low = split(jnp.concatenate(sums, 0))
    table = x_table[...]
    modes = dot(jnp.concatenate([high, low], 1), table[:256]) + dot(high, table[256:])
    real = [None] * 3
    imag = [None] * 3
    for r in range(ROWS):
        cosine, sine = phase[r, 0:1, :], phase[r, 1:2, :]
        for c in range(3):
            re = modes[8 * r : 8 * r + 8, 128 * c : 128 * c + 128]
            im = modes[8 * r : 8 * r + 8, 384 + 128 * c : 512 + 128 * c]
            a = re * cosine + im * sine
            b = im * cosine - re * sine
            real[c] = a if r == 0 else real[c] + a
            imag[c] = b if r == 0 else imag[c] + b
    row = lax.broadcasted_iota(jnp.int32, (8, 128), 0)
    lane = lax.broadcasted_iota(jnp.int32, (8, 128), 1)
    own = ((lane >> 5) & 1) == (row & 1)

    def spread(value):
        value = jnp.where(own, value, pltpu.roll(value, 1, 0))
        return jnp.concatenate([value] * 4, 0)

    weights = w_eff[...]
    mixed_re = None
    for c in range(3):
        cr, ci = spread(real[c]), spread(imag[c])
        wr = weights[32 * c : 32 * c + 32, :128]
        wi = weights[32 * c : 32 * c + 32, 128:]
        a = wr * cr - wi * ci
        b = wr * ci + wi * cr
        mixed_re = a if c == 0 else mixed_re + a
        mixed_im = b if c == 0 else mixed_im + b
    lane = lax.broadcasted_iota(jnp.int32, (32, 128), 1)
    origin = jnp.logical_and(lane == 0, place[0] + place[1] == 0)
    mixed_re = mixed_re + jnp.where(origin, weights[96:128, :128], 0.0)
    mixed_im = mixed_im + jnp.where(origin, weights[96:128, 128:], 0.0)
    turned = jnp.concatenate([mixed_re, mixed_im, mixed_re, mixed_im], 0).T
    blocks = exchange([turned[32 * k : 32 * k + 32] for k in range(4)], 1, 32)
    high, low = split(jnp.concatenate(blocks[:2], 0))
    stack = jnp.concatenate([high, low, high, low], 0)
    out[...] = dot(back_table[...], stack)


def y_kernel(arrived, table, out):
    parts = []
    for group in range(4):
        tiles = [arrived[64 * group + 8 * k : 64 * group + 8 * k + 8, :] for k in range(8)]
        parts.append(exchange(tiles, 0, 1))
    by_x = [jnp.concatenate([parts[g][x] for g in range(4)], 0) for x in range(8)]
    rows = []
    for two in range(4):
        low_ky, high_ky = exchange([by_x[2 * two], by_x[2 * two + 1]], 1, 64)
        data = jnp.concatenate([low_ky, high_ky], 0)
        high = data.astype(BF16).astype(F32)
        rows.append(jnp.concatenate([high, data - high], 0).T.astype(BF16))
    left = jnp.concatenate(rows, 0)
    left = jnp.concatenate([left, left], 1)
    cells = dot(left, table[...])
    for part in range(2):
        for half in range(2):
            lane = 256 * part + 128 * half
            tiles = [cells[64 * x : 64 * x + 64, lane : lane + 128] for x in range(8)]
            for g, block in enumerate(exchange(tiles, 1, 16)):
                out[8 * half + g, 64 * part : 64 * part + 64, :] = block


def local_kernel(combined, advanced, out):
    for o in range(CH):
        out[o] = (
            combined[o, 0] * advanced[0:128, :]
            + combined[o, 1] * advanced[128:256, :]
            + combined[o, 2] * advanced[256:384, :]
            + combined[o, 3]
        )


def z_kernel(arrived, local, table, out):
    block = pl.program_id(0)
    spec = table[...]
    start = pl.multiple_of(block * 8, 8)
    groups = []
    for g in range(8):
        tiles = []
        for k in range(8 * g, 8 * g + 8):
            tiles.append(arrived[k // 4, k % 4, pl.ds(start, 8), :])
        groups.append(exchange(tiles, 0, 1))
    root = math.sqrt(2.0 / math.pi)
    for o in range(8):
        data = jnp.concatenate([groups[g][o] for g in range(8)], 0)
        high = data.astype(BF16).astype(F32)
        left = jnp.concatenate([high, data - high], 0).T.astype(BF16)
        left = jnp.concatenate([left, left], 1)
        value = dot(left, spec) + local[start + o]
        inner = value * (root + (root * 0.044715) * (value * value))
        half = 0.5 * value
        out[o] = (half + half * jnp.tanh(inner)).astype(BF16)


VMEM = pl.BlockSpec(memory_space=pltpu.VMEM)
SMEM = pl.BlockSpec(memory_space=pltpu.SMEM)


def run(kernel, out_shapes, specs, *args, flops=1000000):
    many = isinstance(out_shapes, tuple)
    return pl.pallas_call(
        kernel,
        out_shape=out_shapes,
        in_specs=specs,
        out_specs=tuple(VMEM for _ in out_shapes) if many else VMEM,
        cost_estimate=pl.CostEstimate(flops=flops, transcendentals=0, bytes_accessed=100000),
    )(*args)


def per_device(
    velocity, tendency, step_size, lift_weight, lift_bias, spectral_weight, local_weight, local_bias
):
    highest = lax.Precision.HIGHEST
    place = jnp.stack([lax.axis_index("row"), lax.axis_index("col")]).astype(jnp.int32)
    shape = jax.ShapeDtypeStruct
    advanced, outgoing = run(
        forward_kernel,
        (shape((384, 256), F32), shape((16, 32, 128), F32)),
        [SMEM, SMEM, VMEM, VMEM, VMEM, VMEM, VMEM],
        place,
        step_size,
        velocity.reshape(384, 256),
        tendency.reshape(384, 256),
        z_forward(),
        y_forward(),
        y_phase(),
    )
    arrived = lax.all_to_all(
        outgoing.reshape(256, 2, 128), ("row", "col"), split_axis=0, concat_axis=0, tiled=True
    ).reshape(16, 32, 128)
    lift = jnp.concatenate([lift_weight.T, lift_bias[None]], 0)
    w_eff = run(
        weight_kernel,
        shape((128, 256), F32),
        [VMEM, VMEM],
        spectral_weight.reshape(256, 1024),
        jnp.tile(lift, (1, 32)),
    )
    cells_x = run(
        mix_kernel,
        shape((256, 128), F32),
        [SMEM, VMEM, VMEM, VMEM, VMEM, VMEM],
        place,
        arrived,
        w_eff,
        x_forward(),
        x_phase(),
        x_inverse(),
    )
    by_cells = lax.all_to_all(
        cells_x.reshape(16, 16, 128), "row", split_axis=0, concat_axis=0, tiled=True
    ).reshape(256, 128)
    cells_y = run(y_kernel, shape((16, 128, 128), F32), [VMEM, VMEM], by_cells, y_inverse())
    pencils = lax.all_to_all(cells_y, "col", split_axis=0, concat_axis=0, tiled=True)
    combined = jnp.dot(local_weight, lift_weight, precision=highest)
    offset = jnp.dot(local_weight, lift_bias, precision=highest) + local_bias
    combined = jnp.concatenate([combined, offset[:, None]], 1)
    local = run(local_kernel, shape((32, 128, 256), F32), [SMEM, VMEM], combined, advanced)
    features = pl.pallas_call(
        z_kernel,
        out_shape=shape((32, 128, 256), BF16),
        grid=(4,),
        in_specs=[VMEM, VMEM, VMEM],
        out_specs=pl.BlockSpec((8, 128, 256), lambda i: (i, 0, 0)),
    )(pencils.reshape(16, 4, 32, 128), local, z_inverse())
    return features.reshape(1, 32, 8, 16, 256)


def solution(mesh):
    in_specs = (
        P(None, None, "row", "col", None),
        P(None, None, "row", "col", None),
        P(),
        P(),
        P(),
        P(None, "row", "col", None, None),
        P(),
        P(),
    )
    out_specs = P(None, None, "row", "col", None)
    return jax.shard_map(
        per_device, mesh=mesh, in_specs=in_specs, out_specs=out_specs, check_vma=False
    )
```

```python
import math

import jax
import jax.numpy as jnp
import numpy as np
from jax import lax
from jax.experimental import pallas as pl
from jax.experimental.pallas import tpu as pltpu
from jax.sharding import PartitionSpec as P

NX = 128
NY = 256
NZ = 256
KX = 32
KY = 32
KZ = 32
CH = 32
ROWS = 16
COLS = 16
F32 = jnp.float32
BF16 = jnp.bfloat16


def waves(count):
    index = np.arange(count)
    return np.where(index < count // 2, index, index - count)


def pair(table):
    high = table.astype(np.float32).astype(BF16)
    low = (table - high.astype(np.float64)).astype(np.float32).astype(BF16)
    return high, low


def z_forward():
    angle = 2 * math.pi * ((np.arange(KZ)[:, None] * np.arange(NZ)[None]) % NZ) / NZ
    high, low = pair(np.concatenate([np.cos(angle), -np.sin(angle)], 0))
    return np.concatenate([high, low], 0)


def y_forward():
    angle = 2 * math.pi * ((waves(KY)[:, None] * np.arange(16)[None]) % NY) / NY
    table = np.zeros((8, 16, 2, KY, 8))
    for x in range(8):
        table[x, :, 0, :, x] = np.cos(angle).T
        table[x, :, 1, :, x] = np.sin(angle).T
    high, low = pair(table.reshape(128, 512))
    return np.concatenate([high, high, low], 0)


def y_phase():
    angle = 2 * math.pi * ((waves(KY)[None] * 16 * np.arange(COLS)[:, None]) % NY) / NY
    scale = 1.0 / (NX * NY * NZ)
    table = np.stack([np.cos(angle), np.sin(angle)], 1) * scale
    return np.repeat(table, 8, axis=2).astype(np.float32)


def x_forward():
    angle = 2 * math.pi * ((waves(KX)[None] * np.arange(8)[:, None]) % NX) / NX
    table = np.zeros((4, 2, 2, 8, 2, 3, 2, 2, KX))
    cosine, sine = np.cos(angle), np.sin(angle)
    for c in range(3):
        for e in range(2):
            for d in range(2):
                table[c, 0, e, :, 0, c, e, d] = cosine
                table[c, 1, e, :, 0, c, e, d] = sine
                table[c, 1, e, :, 1, c, e, d] = cosine
                table[c, 0, e, :, 1, c, e, d] = -sine
    high, low = pair(table.reshape(128, 768))
    return np.concatenate([high, high, low], 0)


def x_phase():
    angle = 2 * math.pi * ((waves(KX)[None] * 8 * np.arange(ROWS)[:, None]) % NX) / NX
    table = np.stack([np.cos(angle), np.sin(angle)], 1)
    return np.tile(table, (1, 1, 4)).astype(np.float32)


def x_inverse():
    points = np.arange(NX).reshape(ROWS, 8)
    angle = 2 * math.pi * ((points[:, :, None] * waves(KX)) % NX) / NX
    table = np.zeros((ROWS, 2, 8, 2, KX))
    table[:, 0, :, 0] = np.cos(angle)
    table[:, 0, :, 1] = -np.sin(angle)
    table[:, 1, :, 0] = np.sin(angle)
    table[:, 1, :, 1] = np.cos(angle)
    high, low = pair(table.reshape(256, 64))
    return np.concatenate([high, high, low, low], 1)


def y_inverse():
    angle = 2 * math.pi * ((waves(KY)[:, None] * np.arange(NY)[None]) % NY) / NY
    angle = angle.reshape(ROWS, 2, NY).transpose(1, 0, 2)
    table = np.zeros((2, ROWS, 2, 2, NY))
    table[:, :, 0, 0] = np.cos(angle)
    table[:, :, 1, 0] = -np.sin(angle)
    table[:, :, 0, 1] = np.sin(angle)
    table[:, :, 1, 1] = np.cos(angle)
    high, low = pair(table.reshape(64, 512))
    return np.concatenate([high, high, low, low], 0)


def z_inverse():
    angle = 2 * math.pi * ((np.arange(KZ)[:, None] * np.arange(NZ)[None]) % NZ) / NZ
    double = np.where(np.arange(KZ) == 0, 1.0, 2.0)[:, None]
    angle = angle.reshape(COLS, 2, NZ)
    double = double.reshape(COLS, 2, 1)
    table = np.stack([double * np.cos(angle), -double * np.sin(angle)], 1)
    high, low = pair(table.reshape(64, NZ))
    return np.concatenate([high, high, low, low], 0)


def dot(a, b):
    return jnp.dot(a, b, preferred_element_type=F32)


def dot_t(a, b):
    return lax.dot_general(a, b, (((1,), (1,)), ((), ())), preferred_element_type=F32)


def split(value):
    high = value.astype(BF16)
    low = (value - high.astype(F32)).astype(BF16)
    return high, low


def exchange(arrays, axis, unit):
    arrays = list(arrays)
    length = arrays[0].shape[axis]
    place = lax.broadcasted_iota(jnp.int32, arrays[0].shape, axis)
    bit = 1
    while bit < len(arrays):
        shift = bit * unit
        keep = (place & shift) == 0
        for i in range(len(arrays)):
            if i & bit == 0:
                a, b = arrays[i], arrays[i | bit]
                arrays[i] = jnp.where(keep, a, pltpu.roll(b, shift, axis))
                arrays[i | bit] = jnp.where(keep, pltpu.roll(a, length - shift, axis), b)
        bit *= 2
    return arrays


def forward_kernel(step, velocity, tendency, z_table, y_table, phase, advanced, out):
    value = velocity[...] + step[0] * tendency[...]
    advanced[...] = value
    high, low = split(value)
    first = dot_t(z_table[...], high)
    modes = first[:64] + first[64:] + dot_t(z_table[0:64, :], low)
    modes = jnp.concatenate([modes[:, 128 * c : 128 * c + 128] for c in range(3)], 0)
    high, low = split(modes)
    table = y_table[...]
    sums = dot(jnp.concatenate([high, low], 1), table[:256]) + dot(high, table[256:])
    turn = phase[lax.axis_index("col")]
    cosine, sine = turn[0:1], turn[1:2]
    parts = []
    for c in range(3):
        real = sums[64 * c : 64 * c + 32]
        imag = sums[64 * c + 32 : 64 * c + 64]
        re = real[:, :256] + imag[:, 256:]
        im = imag[:, :256] - real[:, 256:]
        parts.append(re * cosine + im * sine)
        parts.append(im * cosine - re * sine)
    zero = jnp.zeros((32, 128), F32)
    for half in range(2):
        lanes = [p[:, 128 * half : 128 * half + 128] for p in parts] + [zero, zero]
        for g, block in enumerate(exchange(lanes, 1, 16)):
            out[8 * half + g] = block


def prepare_kernel(
    weights, lift, bias, mixing, mixing_bias, advanced, *rest
):
    tables, (w_eff, local), copies, scratch = rest[:5], rest[5:7], rest[7:12], rest[12]
    for source, target in zip(tables, copies):
        target[...] = source[...]
    highest = lax.Precision.HIGHEST
    row = lax.broadcasted_iota(jnp.int32, (32, 1024), 0)
    lane = lax.broadcasted_iota(jnp.int32, (32, 1024), 1)
    spread = jnp.where(row == (lane & 31), 1.0, 0.0).astype(F32)
    same = row == (lane >> 5)
    maps = []
    for j in range(4):
        source = lift[j : j + 1, :] if j < 3 else bias[...]
        source = jnp.broadcast_to(source, (8, 32))
        wide = jnp.dot(source, spread, precision=highest, preferred_element_type=F32)
        maps.append(jnp.where(same, wide[0:1, :], 0.0))
    maps = jnp.concatenate(maps, 0)
    high, rest = split(maps)
    rest = maps - high.astype(F32)
    mid = rest.astype(BF16)
    low = (rest - mid.astype(F32)).astype(BF16)
    w = weights[...]
    w_eff[...] = dot_t(high, w) + dot_t(mid, w) + dot_t(low, w)

    def columns(matrix, vector):
        return lax.dot_general(
            matrix,
            jnp.broadcast_to(vector, (128, 32)),
            (((1,), (1,)), ((), ())),
            precision=highest,
            preferred_element_type=F32,
        )

    local_map = mixing[...]
    eye = jnp.where(
        lax.broadcasted_iota(jnp.int32, (32, 32), 0) == lax.broadcasted_iota(jnp.int32, (32, 32), 1),
        1.0,
        0.0,
    ).astype(F32)
    for j in range(3):
        scratch[j] = columns(local_map, lift[j : j + 1, :])
    scratch[3] = columns(local_map, bias[...]) + columns(eye, mixing_bias[...])

    def body(o, carry):
        scale = [scratch[j, pl.ds(o, 1), :] for j in range(4)]
        for half in range(2):
            lanes = slice(128 * half, 128 * half + 128)
            local[o, :, lanes] = (
                scale[0] * advanced[0:128, lanes]
                + scale[1] * advanced[128:256, lanes]
                + scale[2] * advanced[256:384, lanes]
                + scale[3]
            )
        return carry

    lax.fori_loop(0, CH, body, 0)


def mix_kernel(arrived, w_eff, x_table, phase, back_table, out):
    sums = []
    for r in range(ROWS):
        block = arrived[r]
        total = (block[0:8] + block[8:16]) + (block[16:24] + block[24:32])
        total = total + pltpu.roll(total, 4, 0)
        total = total + pltpu.roll(total, 2, 0)
        sums.append(total)
    high, low = split(jnp.concatenate(sums, 0))
    table = x_table[...]
    modes = dot(jnp.concatenate([high, low], 1), table[:256]) + dot(high, table[256:])
    real = [None] * 3
    imag = [None] * 3
    for r in range(ROWS):
        cosine, sine = phase[r, 0:1, :], phase[r, 1:2, :]
        for c in range(3):
            re = modes[8 * r : 8 * r + 8, 128 * c : 128 * c + 128]
            im = modes[8 * r : 8 * r + 8, 384 + 128 * c : 512 + 128 * c]
            a = re * cosine + im * sine
            b = im * cosine - re * sine
            real[c] = a if r == 0 else real[c] + a
            imag[c] = b if r == 0 else imag[c] + b
    row = lax.broadcasted_iota(jnp.int32, (8, 128), 0)
    lane = lax.broadcasted_iota(jnp.int32, (8, 128), 1)
    own = ((lane >> 5) & 1) == (row & 1)

    def spread(value):
        value = jnp.where(own, value, pltpu.roll(value, 1, 0))
        return jnp.concatenate([value] * 4, 0)

    weights = w_eff[...]
    mixed_re = None
    for c in range(3):
        cr, ci = spread(real[c]), spread(imag[c])
        wr = weights[32 * c : 32 * c + 32, :128]
        wi = weights[32 * c : 32 * c + 32, 128:]
        a = wr * cr - wi * ci
        b = wr * ci + wi * cr
        mixed_re = a if c == 0 else mixed_re + a
        mixed_im = b if c == 0 else mixed_im + b
    lane = lax.broadcasted_iota(jnp.int32, (32, 128), 1)
    origin = jnp.logical_and(lane == 0, lax.axis_index("row") + lax.axis_index("col") == 0)
    mixed_re = mixed_re + jnp.where(origin, weights[96:128, :128], 0.0)
    mixed_im = mixed_im + jnp.where(origin, weights[96:128, 128:], 0.0)
    turned = jnp.concatenate([mixed_re, mixed_im, mixed_re, mixed_im], 0).T
    blocks = exchange([turned[32 * k : 32 * k + 32] for k in range(4)], 1, 32)
    high, low = split(jnp.concatenate(blocks[:2], 0))
    stack = jnp.concatenate([high, low, high, low], 0)
    out[...] = dot(back_table[...], stack)


def y_kernel(arrived, table, out):
    parts = []
    for group in range(4):
        tiles = [arrived[64 * group + 8 * k : 64 * group + 8 * k + 8, :] for k in range(8)]
        parts.append(exchange(tiles, 0, 1))
    by_x = [jnp.concatenate([parts[g][x] for g in range(4)], 0) for x in range(8)]
    rows = []
    for two in range(4):
        low_ky, high_ky = exchange([by_x[2 * two], by_x[2 * two + 1]], 1, 64)
        data = jnp.concatenate([low_ky, high_ky], 0)
        high = data.astype(BF16).astype(F32)
        rows.append(jnp.concatenate([high, data - high], 0).T.astype(BF16))
    left = jnp.concatenate(rows, 0)
    left = jnp.concatenate([left, left], 1)
    cells = dot(left, table[...])
    for part in range(2):
        for half in range(2):
            lane = 256 * part + 128 * half
            tiles = [cells[64 * x : 64 * x + 64, lane : lane + 128] for x in range(8)]
            for g, block in enumerate(exchange(tiles, 1, 16)):
                out[8 * half + g, 64 * part : 64 * part + 64, :] = block


def z_kernel(arrived, local, table, out):
    block = pl.program_id(0)
    spec = table[...]
    start = pl.multiple_of(block * 8, 8)
    groups = []
    for g in range(8):
        tiles = []
        for k in range(8 * g, 8 * g + 8):
            tiles.append(arrived[k // 4, k % 4, pl.ds(start, 8), :])
        groups.append(exchange(tiles, 0, 1))
    root = math.sqrt(2.0 / math.pi)
    for o in range(8):
        data = jnp.concatenate([groups[g][o] for g in range(8)], 0)
        high = data.astype(BF16).astype(F32)
        left = jnp.concatenate([high, data - high], 0).T.astype(BF16)
        left = jnp.concatenate([left, left], 1)
        value = dot(left, spec) + local[start + o]
        inner = value * (root + (root * 0.044715) * (value * value))
        half = 0.5 * value
        out[o] = (half + half * jnp.tanh(inner)).astype(BF16)


VMEM = pl.BlockSpec(memory_space=pltpu.VMEM)
SMEM = pl.BlockSpec(memory_space=pltpu.SMEM)


VMEM = "vmem"
HBM = "hbm"
SMEM = "smem"
BLOCKS = {
    VMEM: pl.BlockSpec(memory_space=pltpu.VMEM),
    HBM: pl.BlockSpec(memory_space=pltpu.VMEM),
    SMEM: pl.BlockSpec(memory_space=pltpu.SMEM),
}


def put(value, where):
    if where == SMEM:
        return value
    space = pltpu.VMEM if where == VMEM else pltpu.HBM
    return pltpu.with_memory_space_constraint(value, space)


def run(kernel, outs, specs, *args, scratch=(), limit=16):
    return pl.pallas_call(
        kernel,
        out_shape=outs,
        in_specs=[BLOCKS[s] for s in specs],
        out_specs=jax.tree.map(lambda _: BLOCKS[VMEM], outs),
        scratch_shapes=scratch,
        compiler_params=pltpu.CompilerParams(vmem_limit_bytes=limit * 1024 * 1024),
        cost_estimate=pl.CostEstimate(flops=1000000, transcendentals=0, bytes_accessed=100000),
    )(*[put(a, s) for a, s in zip(args, specs)])


def per_device(
    velocity, tendency, step_size, lift_weight, lift_bias, spectral_weight, local_weight, local_bias
):
    on_chip = pltpu.VMEM
    advanced, outgoing = run(
        forward_kernel,
        (on_chip((384, 256), F32), on_chip((16, 32, 128), F32)),
        [SMEM] + [HBM] * 5,
        step_size,
        velocity.reshape(384, 256),
        tendency.reshape(384, 256),
        z_forward(),
        y_forward(),
        y_phase(),
    )
    arrived = lax.all_to_all(
        outgoing.reshape(256, 2, 128), ("row", "col"), split_axis=0, concat_axis=0, tiled=True
    ).reshape(16, 32, 128)
    tables = [x_forward(), x_phase(), x_inverse(), y_inverse(), z_inverse()]
    w_eff, local, x_table, turn_table, back_table, y_table, z_table = run(
        prepare_kernel,
        [on_chip((128, 256), F32), on_chip((32, 128, 256), F32)]
        + [on_chip(t.shape, t.dtype) for t in tables],
        [HBM] * 5 + [VMEM] + [HBM] * 5,
        spectral_weight.reshape(256, 1024),
        lift_weight.T,
        lift_bias[None],
        local_weight,
        local_bias[None],
        advanced,
        *tables,
        scratch=(pltpu.VMEM((4, 32, 128), F32),),
    )
    cells_x = run(
        mix_kernel,
        on_chip((256, 128), F32),
        [VMEM] * 5,
        arrived,
        w_eff,
        x_table,
        turn_table,
        back_table,
    )
    by_cells = lax.all_to_all(
        cells_x.reshape(16, 16, 128), "row", split_axis=0, concat_axis=0, tiled=True
    ).reshape(256, 128)
    cells_y = run(y_kernel, on_chip((16, 128, 128), F32), [VMEM, VMEM], by_cells, y_table)
    pencils = lax.all_to_all(cells_y, "col", split_axis=0, concat_axis=0, tiled=True)
    features = pl.pallas_call(
        z_kernel,
        out_shape=jax.ShapeDtypeStruct((32, 128, 256), BF16),
        grid=(4,),
        in_specs=[BLOCKS[VMEM]] * 3,
        out_specs=pl.BlockSpec((8, 128, 256), lambda i: (i, 0, 0)),
        compiler_params=pltpu.CompilerParams(vmem_limit_bytes=16 * 1024 * 1024),
    )(put(pencils.reshape(16, 4, 32, 128), VMEM), put(local, VMEM), put(z_table, VMEM))
    return features.reshape(1, 32, 8, 16, 256)


def solution(mesh):
    in_specs = (
        P(None, None, "row", "col", None),
        P(None, None, "row", "col", None),
        P(),
        P(),
        P(),
        P(None, "row", "col", None, None),
        P(),
        P(),
    )
    out_specs = P(None, None, "row", "col", None)
    return jax.shard_map(
        per_device, mesh=mesh, in_specs=in_specs, out_specs=out_specs, check_vma=False
    )
```

```python
import math

import jax
import jax.numpy as jnp
import numpy as np
from jax import lax
from jax.experimental import pallas as pl
from jax.experimental.pallas import tpu as pltpu
from jax.sharding import PartitionSpec as P

NX = 128
NY = 256
NZ = 256
KX = 32
KY = 32
KZ = 32
CH = 32
ROWS = 16
COLS = 16
F32 = jnp.float32
BF16 = jnp.bfloat16


def waves(count):
    index = np.arange(count)
    return np.where(index < count // 2, index, index - count)


def pair(table):
    high = table.astype(np.float32).astype(BF16)
    low = (table - high.astype(np.float64)).astype(np.float32).astype(BF16)
    return high, low


def z_forward():
    angle = 2 * math.pi * ((np.arange(KZ)[:, None] * np.arange(NZ)[None]) % NZ) / NZ
    high, low = pair(np.concatenate([np.cos(angle), -np.sin(angle)], 0))
    return np.concatenate([high, low], 0)


def y_forward():
    angle = 2 * math.pi * ((waves(KY)[:, None] * np.arange(16)[None]) % NY) / NY
    table = np.zeros((2, 8, 16, 2, KY, 8))
    for x in range(8):
        table[0, x, :, 0, :, x] = np.cos(angle).T
        table[1, x, :, 0, :, x] = np.sin(angle).T
        table[1, x, :, 1, :, x] = np.cos(angle).T
        table[0, x, :, 1, :, x] = -np.sin(angle).T
    high, low = pair(table.reshape(256, 512))
    return np.concatenate([high, low], 0)


def y_phase():
    angle = 2 * math.pi * ((waves(KY)[None] * 16 * np.arange(COLS)[:, None]) % NY) / NY
    scale = 1.0 / (NX * NY * NZ)
    table = np.stack([np.cos(angle), np.sin(angle)], 1) * scale
    return np.repeat(table, 8, axis=2).astype(np.float32)


def x_forward():
    angle = 2 * math.pi * ((waves(KX)[None] * np.arange(8)[:, None]) % NX) / NX
    table = np.zeros((4, 2, 2, 8, 2, 3, 2, 2, KX))
    cosine, sine = np.cos(angle), np.sin(angle)
    for c in range(3):
        for e in range(2):
            for d in range(2):
                table[c, 0, e, :, 0, c, e, d] = cosine
                table[c, 1, e, :, 0, c, e, d] = sine
                table[c, 1, e, :, 1, c, e, d] = cosine
                table[c, 0, e, :, 1, c, e, d] = -sine
    high, low = pair(table.reshape(128, 768))
    return np.concatenate([high, high, low], 0)


def x_phase():
    angle = 2 * math.pi * ((waves(KX)[None] * 8 * np.arange(ROWS)[:, None]) % NX) / NX
    table = np.stack([np.cos(angle), np.sin(angle)], 1)
    return np.tile(table, (1, 1, 4)).astype(np.float32)


def x_inverse():
    points = np.arange(NX).reshape(ROWS, 8)
    angle = 2 * math.pi * ((points[:, :, None] * waves(KX)) % NX) / NX
    table = np.zeros((ROWS, 2, 8, 2, KX))
    table[:, 0, :, 0] = np.cos(angle)
    table[:, 0, :, 1] = -np.sin(angle)
    table[:, 1, :, 0] = np.sin(angle)
    table[:, 1, :, 1] = np.cos(angle)
    high, low = pair(table.reshape(256, 64))
    return np.concatenate([high, high, low, low], 1)


def y_inverse():
    angle = 2 * math.pi * ((waves(KY)[:, None] * np.arange(NY)[None]) % NY) / NY
    angle = angle.reshape(ROWS, 2, NY).transpose(1, 0, 2)
    table = np.zeros((2, ROWS, 2, 2, NY))
    table[:, :, 0, 0] = np.cos(angle)
    table[:, :, 1, 0] = -np.sin(angle)
    table[:, :, 0, 1] = np.sin(angle)
    table[:, :, 1, 1] = np.cos(angle)
    high, low = pair(table.reshape(64, 512))
    return np.concatenate([high, high, low, low], 0)


def z_inverse():
    angle = 2 * math.pi * ((np.arange(KZ)[:, None] * np.arange(NZ)[None]) % NZ) / NZ
    double = np.where(np.arange(KZ) == 0, 0.5, 1.0)[:, None]
    angle = angle.reshape(COLS, 2, NZ)
    double = double.reshape(COLS, 2, 1)
    table = np.stack([double * np.cos(angle), -double * np.sin(angle)], 1)
    high, low = pair(table.reshape(64, NZ))
    return np.concatenate([high, high, low, low], 0)


def dot(a, b):
    return jnp.dot(a, b, preferred_element_type=F32)


def dot_t(a, b):
    return lax.dot_general(a, b, (((1,), (1,)), ((), ())), preferred_element_type=F32)


def split(value):
    high = value.astype(BF16)
    low = (value - high.astype(F32)).astype(BF16)
    return high, low


def exchange(arrays, axis, unit):
    arrays = list(arrays)
    length = arrays[0].shape[axis]
    place = lax.broadcasted_iota(jnp.int32, arrays[0].shape, axis)
    bit = 1
    while bit < len(arrays):
        shift = bit * unit
        keep = (place & shift) == 0
        for i in range(len(arrays)):
            if i & bit == 0:
                a, b = arrays[i], arrays[i | bit]
                arrays[i] = jnp.where(keep, a, pltpu.roll(b, shift, axis))
                arrays[i | bit] = jnp.where(keep, pltpu.roll(a, length - shift, axis), b)
        bit *= 2
    return arrays


def forward_kernel(step, velocity, tendency, z_table, y_table, phase, advanced, out):
    value = velocity[...] + step[0] * tendency[...]
    advanced[...] = value
    high, low = split(value)
    first = dot_t(z_table[...], high)
    modes = first[:64] + first[64:] + dot_t(z_table[0:64, :], low)
    modes = [
        jnp.concatenate([modes[0:32, 128 * c : 128 * c + 128], modes[32:64, 128 * c : 128 * c + 128]], 1)
        for c in range(3)
    ]
    high, low = split(jnp.concatenate(modes, 0))
    first = dot(jnp.concatenate([high, low], 0), y_table[0:256, :])
    sums = first[:96] + first[96:] + dot(high, y_table[256:512, :])
    turn = phase[lax.axis_index("col")]
    cosine, sine = turn[0:1], turn[1:2]
    parts = []
    for c in range(3):
        re = sums[32 * c : 32 * c + 32, :256]
        im = sums[32 * c : 32 * c + 32, 256:]
        parts.append(re * cosine + im * sine)
        parts.append(im * cosine - re * sine)
    zero = jnp.zeros((32, 128), F32)
    for half in range(2):
        lanes = [p[:, 128 * half : 128 * half + 128] for p in parts] + [zero, zero]
        for g, block in enumerate(exchange(lanes, 1, 16)):
            out[8 * half + g] = block


def prepare_kernel(lift, bias, mixing, mixing_bias, advanced, weights, *rest):
    tables, (w_eff, local), copies = rest[:5], rest[5:7], rest[7:12]
    scratch, lines, held_weights, sems = rest[12:]
    loads = [pltpu.make_async_copy(weights, held_weights, sems.at[0])]
    for k, (source, target) in enumerate(zip(tables, copies)):
        loads.append(pltpu.make_async_copy(source, target, sems.at[1 + k]))
    for load in loads:
        load.start()
    highest = lax.Precision.HIGHEST

    def columns(matrix, vector):
        return lax.dot_general(
            matrix,
            jnp.broadcast_to(vector, (128, 32)),
            (((1,), (1,)), ((), ())),
            precision=highest,
            preferred_element_type=F32,
        )

    local_map = mixing[...]
    eye = jnp.where(
        lax.broadcasted_iota(jnp.int32, (32, 32), 0) == lax.broadcasted_iota(jnp.int32, (32, 32), 1),
        1.0,
        0.0,
    ).astype(F32)
    for j in range(3):
        scratch[j] = 0.5 * columns(local_map, lift[j : j + 1, :])
    scratch[3] = 0.5 * (columns(local_map, bias[...]) + columns(eye, mixing_bias[...]))

    def body(o, carry):
        scale = [scratch[j, pl.ds(o, 1), :] for j in range(4)]
        for half in range(2):
            lanes = slice(128 * half, 128 * half + 128)
            lines[o, :, lanes] = (
                scale[0] * advanced[0:128, lanes]
                + scale[1] * advanced[128:256, lanes]
                + scale[2] * advanced[256:384, lanes]
                + scale[3]
            )
        return carry

    for part in range(4):
        lax.fori_loop(8 * part, 8 * part + 8, body, 0)
        chunk = pl.ds(8 * part, 8)
        loads.append(pltpu.make_async_copy(lines.at[chunk], local.at[chunk], sems.at[6 + part]))
        loads[-1].start()
    row = lax.broadcasted_iota(jnp.int32, (32, 1024), 0)
    lane = lax.broadcasted_iota(jnp.int32, (32, 1024), 1)
    spread = jnp.where(row == (lane & 31), 1.0, 0.0).astype(F32)
    same = row == (lane >> 5)
    maps = []
    for j in range(4):
        source = lift[j : j + 1, :] if j < 3 else bias[...]
        source = jnp.broadcast_to(source, (8, 32))
        wide = jnp.dot(source, spread, precision=highest, preferred_element_type=F32)
        maps.append(jnp.where(same, wide[0:1, :], 0.0))
    maps = jnp.concatenate(maps, 0)
    high, rest = split(maps)
    rest = maps - high.astype(F32)
    mid = rest.astype(BF16)
    low = (rest - mid.astype(F32)).astype(BF16)
    loads[0].wait()
    w = held_weights[...]
    w_eff[...] = dot_t(high, w) + dot_t(mid, w) + dot_t(low, w)
    for load in loads[1:]:
        load.wait()


def mix_kernel(arrived, w_eff, x_table, phase, back_table, out):
    sums = []
    for r in range(ROWS):
        block = arrived[r]
        total = (block[0:8] + block[8:16]) + (block[16:24] + block[24:32])
        total = total + pltpu.roll(total, 4, 0)
        total = total + pltpu.roll(total, 2, 0)
        sums.append(total)
    high, low = split(jnp.concatenate(sums, 0))
    table = x_table[...]
    modes = dot(jnp.concatenate([high, low], 1), table[:256]) + dot(high, table[256:])
    real = [None] * 3
    imag = [None] * 3
    for r in range(ROWS):
        cosine, sine = phase[r, 0:1, :], phase[r, 1:2, :]
        for c in range(3):
            re = modes[8 * r : 8 * r + 8, 128 * c : 128 * c + 128]
            im = modes[8 * r : 8 * r + 8, 384 + 128 * c : 512 + 128 * c]
            a = re * cosine + im * sine
            b = im * cosine - re * sine
            real[c] = a if r == 0 else real[c] + a
            imag[c] = b if r == 0 else imag[c] + b
    row = lax.broadcasted_iota(jnp.int32, (8, 128), 0)
    lane = lax.broadcasted_iota(jnp.int32, (8, 128), 1)
    own = ((lane >> 5) & 1) == (row & 1)

    def spread(value):
        value = jnp.where(own, value, pltpu.roll(value, 1, 0))
        return jnp.concatenate([value] * 4, 0)

    weights = w_eff[...]
    mixed_re = None
    for c in range(3):
        cr, ci = spread(real[c]), spread(imag[c])
        wr = weights[32 * c : 32 * c + 32, :128]
        wi = weights[32 * c : 32 * c + 32, 128:]
        a = wr * cr - wi * ci
        b = wr * ci + wi * cr
        mixed_re = a if c == 0 else mixed_re + a
        mixed_im = b if c == 0 else mixed_im + b
    lane = lax.broadcasted_iota(jnp.int32, (32, 128), 1)
    origin = jnp.logical_and(lane == 0, lax.axis_index("row") + lax.axis_index("col") == 0)
    mixed_re = mixed_re + jnp.where(origin, weights[96:128, :128], 0.0)
    mixed_im = mixed_im + jnp.where(origin, weights[96:128, 128:], 0.0)
    turned = jnp.concatenate([mixed_re, mixed_im, mixed_re, mixed_im], 0).T
    blocks = exchange([turned[32 * k : 32 * k + 32] for k in range(4)], 1, 32)
    high, low = split(jnp.concatenate(blocks[:2], 0))
    stack = jnp.concatenate([high, low, high, low], 0)
    out[...] = dot(back_table[...], stack)


def y_kernel(arrived, table, out):
    parts = []
    for group in range(4):
        tiles = [arrived[64 * group + 8 * k : 64 * group + 8 * k + 8, :] for k in range(8)]
        parts.append(exchange(tiles, 0, 1))
    by_x = [jnp.concatenate([parts[g][x] for g in range(4)], 0) for x in range(8)]
    rows = []
    for two in range(4):
        low_ky, high_ky = exchange([by_x[2 * two], by_x[2 * two + 1]], 1, 64)
        data = jnp.concatenate([low_ky, high_ky], 0)
        high = data.astype(BF16).astype(F32)
        rows.append(jnp.concatenate([high, data - high], 0).T.astype(BF16))
    left = jnp.concatenate(rows, 0)
    left = jnp.concatenate([left, left], 1)
    cells = dot(left, table[...])
    for part in range(2):
        for half in range(2):
            lane = 256 * part + 128 * half
            tiles = [cells[64 * x : 64 * x + 64, lane : lane + 128] for x in range(8)]
            for g, block in enumerate(exchange(tiles, 1, 16)):
                out[8 * half + g, 64 * part : 64 * part + 64, :] = block


def z_kernel(arrived, local, table, out, lines, sems):
    spec = table[...]
    root = math.sqrt(2.0 / math.pi)
    stores = []
    for block in range(4):
        groups = []
        for g in range(8):
            tiles = []
            for k in range(8 * g, 8 * g + 8):
                tiles.append(arrived[k // 4, k % 4, 8 * block : 8 * block + 8, :])
            groups.append(exchange(tiles, 0, 1))
        for o in range(8):
            data = jnp.concatenate([groups[g][o] for g in range(8)], 0)
            high = data.astype(BF16).astype(F32)
            left = jnp.concatenate([high, data - high], 0).T.astype(BF16)
            left = jnp.concatenate([left, left], 1)
            half = dot(left, spec) + local[8 * block + o]
            inner = half * (2.0 * root + (8.0 * root * 0.044715) * (half * half))
            lines[8 * block + o] = (half + half * jnp.tanh(inner)).astype(BF16)
            if o % 4 == 3:
                chunk = pl.ds(8 * block + o - 3, 4)
                k = len(stores)
                stores.append(pltpu.make_async_copy(lines.at[chunk], out.at[chunk], sems.at[k]))
                stores[-1].start()
    for store in stores:
        store.wait()


VMEM = "vmem"
HBM = "hbm"
ANY = "any"
SMEM = "smem"
BLOCKS = {
    VMEM: pl.BlockSpec(memory_space=pltpu.VMEM),
    HBM: pl.BlockSpec(memory_space=pltpu.VMEM),
    ANY: pl.BlockSpec(memory_space=pl.ANY),
    SMEM: pl.BlockSpec(memory_space=pltpu.SMEM),
}


def put(value, where):
    if where == SMEM:
        return value
    space = pltpu.VMEM if where == VMEM else pltpu.HBM
    return pltpu.with_memory_space_constraint(value, space)


def run(kernel, outs, specs, *args, scratch=(), limit=16, out_specs=None):
    return pl.pallas_call(
        kernel,
        out_shape=outs,
        in_specs=[BLOCKS[s] for s in specs],
        out_specs=jax.tree.map(lambda _: BLOCKS[VMEM], outs) if out_specs is None else [BLOCKS[o] for o in out_specs],
        scratch_shapes=scratch,
        compiler_params=pltpu.CompilerParams(vmem_limit_bytes=limit * 1024 * 1024),
        cost_estimate=pl.CostEstimate(flops=1000000, transcendentals=0, bytes_accessed=100000),
    )(*[put(a, s) for a, s in zip(args, specs)])


def per_device(
    velocity, tendency, step_size, lift_weight, lift_bias, spectral_weight, local_weight, local_bias
):
    on_chip = pltpu.VMEM
    advanced, outgoing = run(
        forward_kernel,
        (on_chip((384, 256), F32), on_chip((16, 32, 128), F32)),
        [SMEM] + [HBM] * 5,
        step_size,
        velocity.reshape(384, 256),
        tendency.reshape(384, 256),
        z_forward(),
        y_forward(),
        y_phase(),
    )
    arrived = lax.all_to_all(
        outgoing.reshape(256, 1, 256), ("row", "col"), split_axis=0, concat_axis=0, tiled=True
    ).reshape(16, 32, 128)
    tables = [x_forward(), x_phase(), x_inverse(), y_inverse(), z_inverse()]
    w_eff, local, x_table, turn_table, back_table, y_table, z_table = run(
        prepare_kernel,
        [on_chip((128, 256), F32), pltpu.HBM((32, 128, 256), F32)]
        + [on_chip(t.shape, t.dtype) for t in tables],
        [HBM] * 4 + [VMEM] + [ANY] * 6,
        lift_weight.T,
        lift_bias[None],
        local_weight,
        local_bias[None],
        advanced,
        spectral_weight.reshape(256, 1024),
        *tables,
        scratch=(
            pltpu.VMEM((4, 32, 128), F32),
            pltpu.VMEM((32, 128, 256), F32),
            pltpu.VMEM((256, 1024), BF16),
            pltpu.SemaphoreType.DMA((10,)),
        ),
        out_specs=[VMEM, ANY] + [VMEM] * 5,
    )
    cells_x = run(
        mix_kernel,
        on_chip((256, 128), F32),
        [VMEM] * 5,
        arrived,
        w_eff,
        x_table,
        turn_table,
        back_table,
    )
    by_cells = lax.all_to_all(
        cells_x.reshape(16, 16, 128), "row", split_axis=0, concat_axis=0, tiled=True
    ).reshape(256, 128)
    cells_y = run(y_kernel, on_chip((16, 128, 128), F32), [VMEM, VMEM], by_cells, y_table)
    pencils = lax.all_to_all(cells_y, "col", split_axis=0, concat_axis=0, tiled=True)
    (features,) = run(
        z_kernel,
        [jax.ShapeDtypeStruct((32, 128, 256), BF16)],
        [VMEM] * 3,
        pencils.reshape(16, 4, 32, 128),
        local,
        z_table,
        scratch=(pltpu.VMEM((32, 128, 256), BF16), pltpu.SemaphoreType.DMA((8,))),
        out_specs=[ANY],
    )
    return features.reshape(1, 32, 8, 16, 256)


def solution(mesh):
    in_specs = (
        P(None, None, "row", "col", None),
        P(None, None, "row", "col", None),
        P(),
        P(),
        P(),
        P(None, "row", "col", None, None),
        P(),
        P(),
    )
    out_specs = P(None, None, "row", "col", None)
    return jax.shard_map(
        per_device, mesh=mesh, in_specs=in_specs, out_specs=out_specs, check_vma=False
    )
```

```python
import math

import jax
import jax.numpy as jnp
import numpy as np
from jax import lax
from jax.experimental import pallas as pl
from jax.experimental.pallas import tpu as pltpu
from jax.sharding import PartitionSpec as P

NX = 128
NY = 256
NZ = 256
KX = 32
KY = 32
KZ = 32
CH = 32
ROWS = 16
COLS = 16
F32 = jnp.float32
BF16 = jnp.bfloat16


def waves(count):
    index = np.arange(count)
    return np.where(index < count // 2, index, index - count)


def pair(table):
    high = table.astype(np.float32).astype(BF16)
    low = (table - high.astype(np.float64)).astype(np.float32).astype(BF16)
    return high, low


def z_forward():
    angle = 2 * math.pi * ((np.arange(KZ)[:, None] * np.arange(NZ)[None]) % NZ) / NZ
    high, low = pair(np.concatenate([np.cos(angle), -np.sin(angle)], 0))
    return np.concatenate([high, low], 0)


def y_forward():
    angle = 2 * math.pi * ((waves(KY)[:, None] * np.arange(16)[None]) % NY) / NY
    table = np.zeros((2, 8, 16, 2, KY, 8))
    for x in range(8):
        table[0, x, :, 0, :, x] = np.cos(angle).T
        table[1, x, :, 0, :, x] = np.sin(angle).T
        table[1, x, :, 1, :, x] = np.cos(angle).T
        table[0, x, :, 1, :, x] = -np.sin(angle).T
    high, low = pair(table.reshape(256, 512))
    return np.concatenate([high, low], 0)


def y_phase():
    angle = 2 * math.pi * ((waves(KY)[None] * 16 * np.arange(COLS)[:, None]) % NY) / NY
    scale = 1.0 / (NX * NY * NZ)
    table = np.stack([np.cos(angle), np.sin(angle)], 1) * scale
    return np.repeat(table, 8, axis=2).astype(np.float32)


def x_forward():
    angle = 2 * math.pi * ((waves(KX)[None] * np.arange(8)[:, None]) % NX) / NX
    table = np.zeros((4, 2, 2, 8, 2, 3, 2, 2, KX))
    cosine, sine = np.cos(angle), np.sin(angle)
    for c in range(3):
        for e in range(2):
            for d in range(2):
                table[c, 0, e, :, 0, c, e, d] = cosine
                table[c, 1, e, :, 0, c, e, d] = sine
                table[c, 1, e, :, 1, c, e, d] = cosine
                table[c, 0, e, :, 1, c, e, d] = -sine
    high, low = pair(table.reshape(128, 768))
    return np.concatenate([high, high, low], 0)


def x_phase():
    angle = 2 * math.pi * ((waves(KX)[None] * 8 * np.arange(ROWS)[:, None]) % NX) / NX
    table = np.stack([np.cos(angle), np.sin(angle)], 1)
    return np.tile(table, (1, 1, 4)).astype(np.float32)


def x_inverse():
    points = np.arange(NX).reshape(ROWS, 8)
    angle = 2 * math.pi * ((points[:, :, None] * waves(KX)) % NX) / NX
    table = np.zeros((ROWS, 2, 8, 2, KX))
    table[:, 0, :, 0] = np.cos(angle)
    table[:, 0, :, 1] = -np.sin(angle)
    table[:, 1, :, 0] = np.sin(angle)
    table[:, 1, :, 1] = np.cos(angle)
    high, low = pair(table.reshape(256, 64))
    return np.concatenate([high, high, low, low], 1)


def y_inverse():
    angle = 2 * math.pi * ((waves(KY)[:, None] * np.arange(NY)[None]) % NY) / NY
    angle = angle.reshape(ROWS, 2, NY).transpose(1, 0, 2)
    table = np.zeros((2, ROWS, 2, 2, NY))
    table[:, :, 0, 0] = np.cos(angle)
    table[:, :, 1, 0] = -np.sin(angle)
    table[:, :, 0, 1] = np.sin(angle)
    table[:, :, 1, 1] = np.cos(angle)
    high, low = pair(table.reshape(64, 512))
    return np.concatenate([high, high, low, low], 0)


def z_inverse():
    angle = 2 * math.pi * ((np.arange(KZ)[:, None] * np.arange(NZ)[None]) % NZ) / NZ
    double = np.where(np.arange(KZ) == 0, 0.5, 1.0)[:, None]
    angle = angle.reshape(COLS, 2, NZ)
    double = double.reshape(COLS, 2, 1)
    table = np.stack([double * np.cos(angle), -double * np.sin(angle)], 1)
    high, low = pair(table.reshape(64, NZ))
    return np.concatenate([high, high, low, low], 0)


def dot(a, b):
    return jnp.dot(a, b, preferred_element_type=F32)


def dot_t(a, b):
    return lax.dot_general(a, b, (((1,), (1,)), ((), ())), preferred_element_type=F32)


def split(value):
    high = value.astype(BF16)
    low = (value - high.astype(F32)).astype(BF16)
    return high, low


def exchange(arrays, axis, unit):
    count = len(arrays)
    length = count * unit
    place = lax.broadcasted_iota(jnp.int32, arrays[0].shape, axis)
    arrays = [pltpu.roll(a, m * unit, axis) if m else a for m, a in enumerate(arrays)]
    bit = 1
    while bit < count:
        moved = (place & (bit * unit)) != 0
        arrays = [jnp.where(moved, arrays[(k + bit) % count], arrays[k]) for k in range(count)]
        bit *= 2
    return [arrays[0]] + [pltpu.roll(arrays[count - g], length - g * unit, axis) for g in range(1, count)]


def forward_kernel(step, velocity, tendency, z_table, y_table, phase, advanced, out):
    value = velocity[...] + step[0] * tendency[...]
    advanced[...] = value
    high, low = split(value)
    first = dot_t(z_table[...], high)
    modes = first[:64] + first[64:] + dot_t(z_table[0:64, :], low)
    modes = [
        jnp.concatenate([modes[0:32, 128 * c : 128 * c + 128], modes[32:64, 128 * c : 128 * c + 128]], 1)
        for c in range(3)
    ]
    high, low = split(jnp.concatenate(modes, 0))
    first = dot(jnp.concatenate([high, low], 0), y_table[0:256, :])
    sums = first[:96] + first[96:] + dot(high, y_table[256:512, :])
    turn = phase[lax.axis_index("col")]
    cosine, sine = turn[0:1], turn[1:2]
    parts = []
    for c in range(3):
        re = sums[32 * c : 32 * c + 32, :256]
        im = sums[32 * c : 32 * c + 32, 256:]
        parts.append(re * cosine + im * sine)
        parts.append(im * cosine - re * sine)
    zero = jnp.zeros((32, 128), F32)
    for half in range(2):
        lanes = [p[:, 128 * half : 128 * half + 128] for p in parts] + [zero, zero]
        for g, block in enumerate(exchange(lanes, 1, 16)):
            out[8 * half + g] = block


def prepare_kernel(lift, bias, mixing, mixing_bias, advanced, weights, *rest):
    tables, (w_eff, local), copies = rest[:5], rest[5:7], rest[7:12]
    scratch, lines, held_weights, sems = rest[12:]
    loads = [pltpu.make_async_copy(weights, held_weights, sems.at[0])]
    for k, (source, target) in enumerate(zip(tables, copies)):
        loads.append(pltpu.make_async_copy(source, target, sems.at[1 + k]))
    for load in loads:
        load.start()
    highest = lax.Precision.HIGHEST

    def columns(matrix, vector):
        return lax.dot_general(
            matrix,
            jnp.broadcast_to(vector, (128, 32)),
            (((1,), (1,)), ((), ())),
            precision=highest,
            preferred_element_type=F32,
        )

    local_map = mixing[...]
    eye = jnp.where(
        lax.broadcasted_iota(jnp.int32, (32, 32), 0) == lax.broadcasted_iota(jnp.int32, (32, 32), 1),
        1.0,
        0.0,
    ).astype(F32)
    for j in range(3):
        scratch[j] = 0.5 * columns(local_map, lift[j : j + 1, :])
    scratch[3] = 0.5 * (columns(local_map, bias[...]) + columns(eye, mixing_bias[...]))

    def body(o, carry):
        scale = [scratch[j, pl.ds(o, 1), :] for j in range(4)]
        for half in range(2):
            lanes = slice(128 * half, 128 * half + 128)
            lines[o, :, lanes] = (
                scale[0] * advanced[0:128, lanes]
                + scale[1] * advanced[128:256, lanes]
                + scale[2] * advanced[256:384, lanes]
                + scale[3]
            )
        return carry

    for part in range(4):
        lax.fori_loop(8 * part, 8 * part + 8, body, 0)
        chunk = pl.ds(8 * part, 8)
        loads.append(pltpu.make_async_copy(lines.at[chunk], local.at[chunk], sems.at[6 + part]))
        loads[-1].start()
    row = lax.broadcasted_iota(jnp.int32, (32, 1024), 0)
    lane = lax.broadcasted_iota(jnp.int32, (32, 1024), 1)
    spread = jnp.where(row == (lane & 31), 1.0, 0.0).astype(F32)
    same = row == (lane >> 5)
    maps = []
    for j in range(4):
        source = lift[j : j + 1, :] if j < 3 else bias[...]
        source = jnp.broadcast_to(source, (8, 32))
        wide = jnp.dot(source, spread, precision=highest, preferred_element_type=F32)
        maps.append(jnp.where(same, wide[0:1, :], 0.0))
    maps = jnp.concatenate(maps, 0)
    high, rest = split(maps)
    rest = maps - high.astype(F32)
    mid = rest.astype(BF16)
    low = (rest - mid.astype(F32)).astype(BF16)
    loads[0].wait()
    w = held_weights[...]
    w_eff[...] = dot_t(high, w) + dot_t(mid, w) + dot_t(low, w)
    for load in loads[1:]:
        load.wait()


def mix_kernel(arrived, w_eff, x_table, phase, back_table, out):
    sums = []
    for r in range(ROWS):
        block = arrived[r]
        total = (block[0:8] + block[8:16]) + (block[16:24] + block[24:32])
        total = total + pltpu.roll(total, 4, 0)
        total = total + pltpu.roll(total, 2, 0)
        sums.append(total)
    high, low = split(jnp.concatenate(sums, 0))
    table = x_table[...]
    modes = dot(jnp.concatenate([high, low], 1), table[:256]) + dot(high, table[256:])
    real = [None] * 3
    imag = [None] * 3
    for r in range(ROWS):
        cosine, sine = phase[r, 0:1, :], phase[r, 1:2, :]
        for c in range(3):
            re = modes[8 * r : 8 * r + 8, 128 * c : 128 * c + 128]
            im = modes[8 * r : 8 * r + 8, 384 + 128 * c : 512 + 128 * c]
            a = re * cosine + im * sine
            b = im * cosine - re * sine
            real[c] = a if r == 0 else real[c] + a
            imag[c] = b if r == 0 else imag[c] + b
    row = lax.broadcasted_iota(jnp.int32, (8, 128), 0)
    lane = lax.broadcasted_iota(jnp.int32, (8, 128), 1)
    own = ((lane >> 5) & 1) == (row & 1)

    def spread(value):
        value = jnp.where(own, value, pltpu.roll(value, 1, 0))
        return jnp.concatenate([value] * 4, 0)

    weights = w_eff[...]
    mixed_re = None
    for c in range(3):
        cr, ci = spread(real[c]), spread(imag[c])
        wr = weights[32 * c : 32 * c + 32, :128]
        wi = weights[32 * c : 32 * c + 32, 128:]
        a = wr * cr - wi * ci
        b = wr * ci + wi * cr
        mixed_re = a if c == 0 else mixed_re + a
        mixed_im = b if c == 0 else mixed_im + b
    lane = lax.broadcasted_iota(jnp.int32, (32, 128), 1)
    origin = jnp.logical_and(lane == 0, lax.axis_index("row") + lax.axis_index("col") == 0)
    mixed_re = mixed_re + jnp.where(origin, weights[96:128, :128], 0.0)
    mixed_im = mixed_im + jnp.where(origin, weights[96:128, 128:], 0.0)
    turned = jnp.concatenate([mixed_re, mixed_im, mixed_re, mixed_im], 0).T
    blocks = exchange([turned[32 * k : 32 * k + 32] for k in range(4)], 1, 32)
    high, low = split(jnp.concatenate(blocks[:2], 0))
    stack = jnp.concatenate([high, low, high, low], 0)
    out[...] = dot(back_table[...], stack)


def y_kernel(arrived, table, out):
    parts = []
    for group in range(4):
        tiles = [arrived[64 * group + 8 * k : 64 * group + 8 * k + 8, :] for k in range(8)]
        parts.append(exchange(tiles, 0, 1))
    by_x = [jnp.concatenate([parts[g][x] for g in range(4)], 0) for x in range(8)]
    rows = []
    for two in range(4):
        low_ky, high_ky = exchange([by_x[2 * two], by_x[2 * two + 1]], 1, 64)
        data = jnp.concatenate([low_ky, high_ky], 0)
        high = data.astype(BF16).astype(F32)
        rows.append(jnp.concatenate([high, data - high], 0).T.astype(BF16))
    left = jnp.concatenate(rows, 0)
    left = jnp.concatenate([left, left], 1)
    for part in range(2):
        for half in range(2):
            lane = 256 * part + 128 * half
            cells = dot(left, table[:, lane : lane + 128])
            tiles = [cells[64 * x : 64 * x + 64] for x in range(8)]
            for g, block in enumerate(exchange(tiles, 1, 16)):
                out[8 * half + g, 64 * part : 64 * part + 64, :] = block


def z_kernel(arrived, local, table, out, lines, sems):
    spec = table[...]
    root = math.sqrt(2.0 / math.pi)
    stores = []
    for block in range(4):
        groups = []
        for g in range(8):
            tiles = []
            for k in range(8 * g, 8 * g + 8):
                tiles.append(arrived[k // 4, k % 4, 8 * block : 8 * block + 8, :])
            groups.append(exchange(tiles, 0, 1))
        for o in range(8):
            data = jnp.concatenate([groups[g][o] for g in range(8)], 0)
            high = data.astype(BF16).astype(F32)
            left = jnp.concatenate([high, data - high], 0).T.astype(BF16)
            left = jnp.concatenate([left, left], 1)
            half = dot(left, spec) + local[8 * block + o]
            inner = half * (2.0 * root + (8.0 * root * 0.044715) * (half * half))
            lines[8 * block + o] = (half + half * jnp.tanh(inner)).astype(BF16)
            if o % 4 == 3:
                chunk = pl.ds(8 * block + o - 3, 4)
                k = len(stores)
                stores.append(pltpu.make_async_copy(lines.at[chunk], out.at[chunk], sems.at[k]))
                stores[-1].start()
    for store in stores:
        store.wait()


VMEM = "vmem"
HBM = "hbm"
ANY = "any"
SMEM = "smem"
BLOCKS = {
    VMEM: pl.BlockSpec(memory_space=pltpu.VMEM),
    HBM: pl.BlockSpec(memory_space=pltpu.VMEM),
    ANY: pl.BlockSpec(memory_space=pl.ANY),
    SMEM: pl.BlockSpec(memory_space=pltpu.SMEM),
}


def put(value, where):
    if where == SMEM:
        return value
    space = pltpu.VMEM if where == VMEM else pltpu.HBM
    return pltpu.with_memory_space_constraint(value, space)


def run(kernel, outs, specs, *args, scratch=(), limit=16, out_specs=None):
    return pl.pallas_call(
        kernel,
        out_shape=outs,
        in_specs=[BLOCKS[s] for s in specs],
        out_specs=jax.tree.map(lambda _: BLOCKS[VMEM], outs) if out_specs is None else [BLOCKS[o] for o in out_specs],
        scratch_shapes=scratch,
        compiler_params=pltpu.CompilerParams(vmem_limit_bytes=limit * 1024 * 1024),
        cost_estimate=pl.CostEstimate(flops=1000000, transcendentals=0, bytes_accessed=100000),
    )(*[put(a, s) for a, s in zip(args, specs)])


def per_device(
    velocity, tendency, step_size, lift_weight, lift_bias, spectral_weight, local_weight, local_bias
):
    on_chip = pltpu.VMEM
    advanced, outgoing = run(
        forward_kernel,
        (on_chip((384, 256), F32), on_chip((16, 32, 128), F32)),
        [SMEM] + [HBM] * 5,
        step_size,
        velocity.reshape(384, 256),
        tendency.reshape(384, 256),
        z_forward(),
        y_forward(),
        y_phase(),
    )
    arrived = lax.all_to_all(
        outgoing.reshape(256, 1, 256), ("row", "col"), split_axis=0, concat_axis=0, tiled=True
    ).reshape(16, 32, 128)
    tables = [x_forward(), x_phase(), x_inverse(), y_inverse(), z_inverse()]
    w_eff, local, x_table, turn_table, back_table, y_table, z_table = run(
        prepare_kernel,
        [on_chip((128, 256), F32), pltpu.HBM((32, 128, 256), F32)]
        + [on_chip(t.shape, t.dtype) for t in tables],
        [HBM] * 4 + [VMEM] + [ANY] * 6,
        lift_weight.T,
        lift_bias[None],
        local_weight,
        local_bias[None],
        advanced,
        spectral_weight.reshape(256, 1024),
        *tables,
        scratch=(
            pltpu.VMEM((4, 32, 128), F32),
            pltpu.VMEM((32, 128, 256), F32),
            pltpu.VMEM((256, 1024), BF16),
            pltpu.SemaphoreType.DMA((10,)),
        ),
        out_specs=[VMEM, ANY] + [VMEM] * 5,
    )
    cells_x = run(
        mix_kernel,
        on_chip((256, 128), F32),
        [VMEM] * 5,
        arrived,
        w_eff,
        x_table,
        turn_table,
        back_table,
    )
    by_cells = lax.all_to_all(
        cells_x.reshape(16, 16, 128), "row", split_axis=0, concat_axis=0, tiled=True
    ).reshape(256, 128)
    cells_y = run(y_kernel, on_chip((16, 128, 128), F32), [VMEM, VMEM], by_cells, y_table)
    pencils = lax.all_to_all(cells_y, "col", split_axis=0, concat_axis=0, tiled=True)
    (features,) = run(
        z_kernel,
        [jax.ShapeDtypeStruct((32, 128, 256), BF16)],
        [VMEM] * 3,
        pencils.reshape(16, 4, 32, 128),
        local,
        z_table,
        scratch=(pltpu.VMEM((32, 128, 256), BF16), pltpu.SemaphoreType.DMA((8,))),
        out_specs=[ANY],
    )
    return features.reshape(1, 32, 8, 16, 256)


def solution(mesh):
    in_specs = (
        P(None, None, "row", "col", None),
        P(None, None, "row", "col", None),
        P(),
        P(),
        P(),
        P(None, "row", "col", None, None),
        P(),
        P(),
    )
    out_specs = P(None, None, "row", "col", None)
    return jax.shard_map(
        per_device, mesh=mesh, in_specs=in_specs, out_specs=out_specs, check_vma=False
    )
```

```python
import math

import jax
import jax.numpy as jnp
import numpy as np
from jax import lax
from jax.experimental import pallas as pl
from jax.experimental.pallas import tpu as pltpu
from jax.sharding import PartitionSpec as P

NX = 128
NY = 256
NZ = 256
KX = 32
KY = 32
KZ = 32
CH = 32
ROWS = 16
COLS = 16
SNAKE = [4 * i + (j if i % 2 == 0 else 3 - j) for i in range(4) for j in range(4)]
F32 = jnp.float32
BF16 = jnp.bfloat16


def waves(count):
    index = np.arange(count)
    return np.where(index < count // 2, index, index - count)


def pair(table):
    high = table.astype(np.float32).astype(BF16)
    low = (table - high.astype(np.float64)).astype(np.float32).astype(BF16)
    return high, low


def z_forward():
    angle = 2 * math.pi * ((np.arange(KZ)[:, None] * np.arange(NZ)[None]) % NZ) / NZ
    high, low = pair(np.concatenate([np.cos(angle), -np.sin(angle)], 0))
    return np.concatenate([high, low], 0)


def y_forward():
    angle = 2 * math.pi * ((waves(KY)[:, None] * np.arange(16)[None]) % NY) / NY
    table = np.zeros((2, 8, 16, 2, KY, 8))
    for x in range(8):
        table[0, x, :, 0, :, x] = np.cos(angle).T
        table[1, x, :, 0, :, x] = np.sin(angle).T
        table[1, x, :, 1, :, x] = np.cos(angle).T
        table[0, x, :, 1, :, x] = -np.sin(angle).T
    high, low = pair(table.reshape(256, 512))
    return np.concatenate([high, low], 0)


def y_phase():
    angle = 2 * math.pi * ((waves(KY)[None] * 16 * np.arange(COLS)[:, None]) % NY) / NY
    scale = 1.0 / (NX * NY * NZ)
    table = np.stack([np.cos(angle), np.sin(angle)], 1) * scale
    return np.repeat(table, 8, axis=2).astype(np.float32)


def x_forward():
    angle = 2 * math.pi * ((waves(KX)[None] * np.arange(8)[:, None]) % NX) / NX
    table = np.zeros((4, 2, 2, 8, 2, 3, 2, 2, KX))
    cosine, sine = np.cos(angle), np.sin(angle)
    for c in range(3):
        for e in range(2):
            for d in range(2):
                table[c, 0, e, :, 0, c, e, d] = cosine
                table[c, 1, e, :, 0, c, e, d] = sine
                table[c, 1, e, :, 1, c, e, d] = cosine
                table[c, 0, e, :, 1, c, e, d] = -sine
    high, low = pair(table.reshape(128, 768))
    return np.concatenate([high, high, low], 0)


def x_phase():
    angle = 2 * math.pi * ((waves(KX)[None] * 8 * np.arange(ROWS)[:, None]) % NX) / NX
    table = np.stack([np.cos(angle), np.sin(angle)], 1)
    return np.tile(table, (1, 1, 4)).astype(np.float32)


def x_inverse():
    points = np.arange(NX).reshape(ROWS, 8)
    angle = 2 * math.pi * ((points[:, :, None] * waves(KX)) % NX) / NX
    table = np.zeros((ROWS, 2, 8, 2, KX))
    table[:, 0, :, 0] = np.cos(angle)
    table[:, 0, :, 1] = -np.sin(angle)
    table[:, 1, :, 0] = np.sin(angle)
    table[:, 1, :, 1] = np.cos(angle)
    high, low = pair(table.reshape(256, 64))
    return np.concatenate([high, high, low, low], 1)


def y_inverse():
    angle = 2 * math.pi * ((waves(KY)[:, None] * np.arange(NY)[None]) % NY) / NY
    angle = angle.reshape(ROWS, 2, COLS, 16)[:, :, SNAKE].reshape(ROWS, 2, NY).transpose(1, 0, 2)
    table = np.zeros((2, ROWS, 2, 2, NY))
    table[:, :, 0, 0] = np.cos(angle)
    table[:, :, 1, 0] = -np.sin(angle)
    table[:, :, 0, 1] = np.sin(angle)
    table[:, :, 1, 1] = np.cos(angle)
    high, low = pair(table.reshape(64, 512))
    return np.concatenate([high, high, low, low], 0)


def z_inverse():
    angle = 2 * math.pi * ((np.arange(KZ)[:, None] * np.arange(NZ)[None]) % NZ) / NZ
    double = np.where(np.arange(KZ) == 0, 0.5, 1.0)[:, None]
    angle = angle.reshape(COLS, 2, NZ)[SNAKE]
    double = double.reshape(COLS, 2, 1)[SNAKE]
    table = np.stack([double * np.cos(angle), -double * np.sin(angle)], 1)
    high, low = pair(table.reshape(64, NZ))
    return np.concatenate([high, high, low, low], 0)


def dot(a, b):
    return jnp.dot(a, b, preferred_element_type=F32)


def dot_t(a, b):
    return lax.dot_general(a, b, (((1,), (1,)), ((), ())), preferred_element_type=F32)


def split(value):
    high = value.astype(BF16)
    low = (value - high.astype(F32)).astype(BF16)
    return high, low


def exchange(arrays, axis, unit):
    count = len(arrays)
    length = count * unit
    place = lax.broadcasted_iota(jnp.int32, arrays[0].shape, axis)
    arrays = [pltpu.roll(a, m * unit, axis) if m else a for m, a in enumerate(arrays)]
    bit = 1
    while bit < count:
        moved = (place & (bit * unit)) != 0
        arrays = [jnp.where(moved, arrays[(k + bit) % count], arrays[k]) for k in range(count)]
        bit *= 2
    return [arrays[0]] + [pltpu.roll(arrays[count - g], length - g * unit, axis) for g in range(1, count)]


def forward_kernel(step, velocity, tendency, z_table, y_table, phase, advanced, out):
    value = velocity[...] + step[0] * tendency[...]
    advanced[...] = value
    high, low = split(value)
    first = dot_t(z_table[...], high)
    modes = first[:64] + first[64:] + dot_t(z_table[0:64, :], low)
    modes = [
        jnp.concatenate([modes[0:32, 128 * c : 128 * c + 128], modes[32:64, 128 * c : 128 * c + 128]], 1)
        for c in range(3)
    ]
    high, low = split(jnp.concatenate(modes, 0))
    first = dot(jnp.concatenate([high, low], 0), y_table[0:256, :])
    sums = first[:96] + first[96:] + dot(high, y_table[256:512, :])
    turn = phase[lax.axis_index("col")]
    cosine, sine = turn[0:1], turn[1:2]
    parts = []
    for c in range(3):
        re = sums[32 * c : 32 * c + 32, :256]
        im = sums[32 * c : 32 * c + 32, 256:]
        parts.append(re * cosine + im * sine)
        parts.append(im * cosine - re * sine)
    zero = jnp.zeros((32, 128), F32)
    for half in range(2):
        lanes = [p[:, 128 * half : 128 * half + 128] for p in parts] + [zero, zero]
        for g, block in enumerate(exchange(lanes, 1, 16)):
            out[8 * half + g] = block


def prepare_kernel(lift, bias, mixing, mixing_bias, advanced, weights, *rest):
    tables, (w_eff, local), copies = rest[:5], rest[5:7], rest[7:12]
    scratch, lines, held_weights, sems = rest[12:]
    loads = [pltpu.make_async_copy(weights, held_weights, sems.at[0])]
    for k, (source, target) in enumerate(zip(tables, copies)):
        loads.append(pltpu.make_async_copy(source, target, sems.at[1 + k]))
    for load in loads:
        load.start()
    highest = lax.Precision.HIGHEST

    def columns(matrix, vector):
        return lax.dot_general(
            matrix,
            jnp.broadcast_to(vector, (128, 32)),
            (((1,), (1,)), ((), ())),
            precision=highest,
            preferred_element_type=F32,
        )

    local_map = mixing[...]
    eye = jnp.where(
        lax.broadcasted_iota(jnp.int32, (32, 32), 0) == lax.broadcasted_iota(jnp.int32, (32, 32), 1),
        1.0,
        0.0,
    ).astype(F32)
    for j in range(3):
        scratch[j] = 0.5 * columns(local_map, lift[j : j + 1, :])
    scratch[3] = 0.5 * (columns(local_map, bias[...]) + columns(eye, mixing_bias[...]))

    def body(o, carry):
        scale = [scratch[j, pl.ds(o, 1), :] for j in range(4)]
        for half in range(2):
            lanes = slice(128 * half, 128 * half + 128)
            lines[o, :, lanes] = (
                scale[0] * advanced[0:128, lanes]
                + scale[1] * advanced[128:256, lanes]
                + scale[2] * advanced[256:384, lanes]
                + scale[3]
            )
        return carry

    for part in range(4):
        lax.fori_loop(8 * part, 8 * part + 8, body, 0)
        chunk = pl.ds(8 * part, 8)
        loads.append(pltpu.make_async_copy(lines.at[chunk], local.at[chunk], sems.at[6 + part]))
        loads[-1].start()
    row = lax.broadcasted_iota(jnp.int32, (32, 1024), 0)
    lane = lax.broadcasted_iota(jnp.int32, (32, 1024), 1)
    spread = jnp.where(row == (lane & 31), 1.0, 0.0).astype(F32)
    same = row == (lane >> 5)
    maps = []
    for j in range(4):
        source = lift[j : j + 1, :] if j < 3 else bias[...]
        source = jnp.broadcast_to(source, (8, 32))
        wide = jnp.dot(source, spread, precision=highest, preferred_element_type=F32)
        maps.append(jnp.where(same, wide[0:1, :], 0.0))
    maps = jnp.concatenate(maps, 0)
    high, rest = split(maps)
    rest = maps - high.astype(F32)
    mid = rest.astype(BF16)
    low = (rest - mid.astype(F32)).astype(BF16)
    loads[0].wait()
    w = held_weights[...]
    w_eff[...] = dot_t(high, w) + dot_t(mid, w) + dot_t(low, w)
    for load in loads[1:]:
        load.wait()


def mix_kernel(arrived, w_eff, x_table, phase, back_table, out):
    sums = []
    for r in range(ROWS):
        block = arrived[r]
        total = (block[0:8] + block[8:16]) + (block[16:24] + block[24:32])
        total = total + pltpu.roll(total, 4, 0)
        total = total + pltpu.roll(total, 2, 0)
        sums.append(total)
    high, low = split(jnp.concatenate(sums, 0))
    table = x_table[...]
    modes = dot(jnp.concatenate([high, low], 1), table[:256]) + dot(high, table[256:])
    real = [None] * 3
    imag = [None] * 3
    for r in range(ROWS):
        cosine, sine = phase[r, 0:1, :], phase[r, 1:2, :]
        for c in range(3):
            re = modes[8 * r : 8 * r + 8, 128 * c : 128 * c + 128]
            im = modes[8 * r : 8 * r + 8, 384 + 128 * c : 512 + 128 * c]
            a = re * cosine + im * sine
            b = im * cosine - re * sine
            real[c] = a if r == 0 else real[c] + a
            imag[c] = b if r == 0 else imag[c] + b
    row = lax.broadcasted_iota(jnp.int32, (8, 128), 0)
    lane = lax.broadcasted_iota(jnp.int32, (8, 128), 1)
    own = ((lane >> 5) & 1) == (row & 1)

    def spread(value):
        value = jnp.where(own, value, pltpu.roll(value, 1, 0))
        return jnp.concatenate([value] * 4, 0)

    weights = w_eff[...]
    mixed_re = None
    for c in range(3):
        cr, ci = spread(real[c]), spread(imag[c])
        wr = weights[32 * c : 32 * c + 32, :128]
        wi = weights[32 * c : 32 * c + 32, 128:]
        a = wr * cr - wi * ci
        b = wr * ci + wi * cr
        mixed_re = a if c == 0 else mixed_re + a
        mixed_im = b if c == 0 else mixed_im + b
    lane = lax.broadcasted_iota(jnp.int32, (32, 128), 1)
    origin = jnp.logical_and(lane == 0, lax.axis_index("row") + lax.axis_index("col") == 0)
    mixed_re = mixed_re + jnp.where(origin, weights[96:128, :128], 0.0)
    mixed_im = mixed_im + jnp.where(origin, weights[96:128, 128:], 0.0)
    turned = jnp.concatenate([mixed_re, mixed_im, mixed_re, mixed_im], 0).T
    blocks = exchange([turned[32 * k : 32 * k + 32] for k in range(4)], 1, 32)
    high, low = split(jnp.concatenate(blocks[:2], 0))
    stack = jnp.concatenate([high, low, high, low], 0)
    out[...] = dot(back_table[...], stack)


def y_kernel(arrived, table, out):
    parts = []
    for group in range(4):
        tiles = [arrived[64 * group + 8 * k : 64 * group + 8 * k + 8, :] for k in range(8)]
        parts.append(exchange(tiles, 0, 1))
    by_x = [jnp.concatenate([parts[g][x] for g in range(4)], 0) for x in range(8)]
    rows = []
    for two in range(4):
        low_ky, high_ky = exchange([by_x[2 * two], by_x[2 * two + 1]], 1, 64)
        data = jnp.concatenate([low_ky, high_ky], 0)
        high = data.astype(BF16).astype(F32)
        rows.append(jnp.concatenate([high, data - high], 0).T.astype(BF16))
    left = jnp.concatenate(rows, 0)
    left = jnp.concatenate([left, left], 1)
    for part in range(2):
        for half in range(2):
            lane = 256 * part + 128 * half
            cells = dot(left, table[:, lane : lane + 128])
            tiles = [cells[64 * x : 64 * x + 64] for x in range(8)]
            for g, block in enumerate(exchange(tiles, 1, 16)):
                out[8 * half + g, 64 * part : 64 * part + 64, :] = block


def z_kernel(arrived, local, table, out, lines, sems):
    spec = table[...]
    root = math.sqrt(2.0 / math.pi)
    stores = []
    for block in range(4):
        groups = []
        for g in range(8):
            tiles = []
            for k in range(8 * g, 8 * g + 8):
                tiles.append(arrived[k // 4, k % 4, 8 * block : 8 * block + 8, :])
            groups.append(exchange(tiles, 0, 1))
        for o in range(8):
            data = jnp.concatenate([groups[g][o] for g in range(8)], 0)
            high = data.astype(BF16).astype(F32)
            left = jnp.concatenate([high, data - high], 0).T.astype(BF16)
            left = jnp.concatenate([left, left], 1)
            half = dot(left, spec) + local[8 * block + o]
            inner = half * (2.0 * root + (8.0 * root * 0.044715) * (half * half))
            lines[8 * block + o] = (half + half * jnp.tanh(inner)).astype(BF16)
            if o % 4 == 3:
                chunk = pl.ds(8 * block + o - 3, 4)
                k = len(stores)
                stores.append(pltpu.make_async_copy(lines.at[chunk], out.at[chunk], sems.at[k]))
                stores[-1].start()
    for store in stores:
        store.wait()


VMEM = "vmem"
HBM = "hbm"
ANY = "any"
SMEM = "smem"
BLOCKS = {
    VMEM: pl.BlockSpec(memory_space=pltpu.VMEM),
    HBM: pl.BlockSpec(memory_space=pltpu.VMEM),
    ANY: pl.BlockSpec(memory_space=pl.ANY),
    SMEM: pl.BlockSpec(memory_space=pltpu.SMEM),
}


def put(value, where):
    if where == SMEM:
        return value
    space = pltpu.VMEM if where == VMEM else pltpu.HBM
    return pltpu.with_memory_space_constraint(value, space)


def run(kernel, outs, specs, *args, scratch=(), limit=16, out_specs=None):
    return pl.pallas_call(
        kernel,
        out_shape=outs,
        in_specs=[BLOCKS[s] for s in specs],
        out_specs=jax.tree.map(lambda _: BLOCKS[VMEM], outs) if out_specs is None else [BLOCKS[o] for o in out_specs],
        scratch_shapes=scratch,
        compiler_params=pltpu.CompilerParams(vmem_limit_bytes=limit * 1024 * 1024),
        cost_estimate=pl.CostEstimate(flops=1000000, transcendentals=0, bytes_accessed=100000),
    )(*[put(a, s) for a, s in zip(args, specs)])


def per_device(
    velocity, tendency, step_size, lift_weight, lift_bias, spectral_weight, local_weight, local_bias
):
    on_chip = pltpu.VMEM
    advanced, outgoing = run(
        forward_kernel,
        (on_chip((384, 256), F32), on_chip((16, 32, 128), F32)),
        [SMEM] + [HBM] * 5,
        step_size,
        velocity.reshape(384, 256),
        tendency.reshape(384, 256),
        z_forward(),
        y_forward(),
        y_phase(),
    )
    arrived = lax.all_to_all(
        outgoing.reshape(256, 1, 256), ("row", "col"), split_axis=0, concat_axis=0, tiled=True
    ).reshape(16, 32, 128)
    tables = [x_forward(), x_phase(), x_inverse(), y_inverse(), z_inverse()]
    w_eff, local, x_table, turn_table, back_table, y_table, z_table = run(
        prepare_kernel,
        [on_chip((128, 256), F32), pltpu.HBM((32, 128, 256), F32)]
        + [on_chip(t.shape, t.dtype) for t in tables],
        [HBM] * 4 + [VMEM] + [ANY] * 6,
        lift_weight.T,
        lift_bias[None],
        local_weight,
        local_bias[None],
        advanced,
        spectral_weight.reshape(256, 1024),
        *tables,
        scratch=(
            pltpu.VMEM((4, 32, 128), F32),
            pltpu.VMEM((32, 128, 256), F32),
            pltpu.VMEM((256, 1024), BF16),
            pltpu.SemaphoreType.DMA((10,)),
        ),
        out_specs=[VMEM, ANY] + [VMEM] * 5,
    )
    cells_x = run(
        mix_kernel,
        on_chip((256, 128), F32),
        [VMEM] * 5,
        arrived,
        w_eff,
        x_table,
        turn_table,
        back_table,
    )
    by_cells = lax.all_to_all(
        cells_x.reshape(16, 16, 128), "row", split_axis=0, concat_axis=0, tiled=True
    ).reshape(256, 128)
    cells_y = run(y_kernel, on_chip((16, 128, 128), F32), [VMEM, VMEM], by_cells, y_table)
    pencils = lax.all_to_all(
        cells_y, "col", split_axis=0, concat_axis=0, tiled=True, axis_index_groups=[SNAKE]
    )
    (features,) = run(
        z_kernel,
        [jax.ShapeDtypeStruct((32, 128, 256), BF16)],
        [VMEM] * 3,
        pencils.reshape(16, 4, 32, 128),
        local,
        z_table,
        scratch=(pltpu.VMEM((32, 128, 256), BF16), pltpu.SemaphoreType.DMA((8,))),
        out_specs=[ANY],
    )
    return features.reshape(1, 32, 8, 16, 256)


def solution(mesh):
    in_specs = (
        P(None, None, "row", "col", None),
        P(None, None, "row", "col", None),
        P(),
        P(),
        P(),
        P(None, "row", "col", None, None),
        P(),
        P(),
    )
    out_specs = P(None, None, "row", "col", None)
    return jax.shard_map(
        per_device, mesh=mesh, in_specs=in_specs, out_specs=out_specs, check_vma=False
    )
```

```python
import math

import jax
import jax.numpy as jnp
import numpy as np
from jax import lax
from jax.experimental import pallas as pl
from jax.experimental.pallas import tpu as pltpu
from jax.sharding import PartitionSpec as P

NX = 128
NY = 256
NZ = 256
KX = 32
KY = 32
KZ = 32
CH = 32
ROWS = 16
COLS = 16
SNAKE = [4 * i + (j if i % 2 == 0 else 3 - j) for i in range(4) for j in range(4)]
CHAIN = [2 * z for z in range(8)] + [2 * z + 1 for z in range(7, -1, -1)]
F32 = jnp.float32
BF16 = jnp.bfloat16


def waves(count):
    index = np.arange(count)
    return np.where(index < count // 2, index, index - count)


def pair(table):
    high = table.astype(np.float32).astype(BF16)
    low = (table - high.astype(np.float64)).astype(np.float32).astype(BF16)
    return high, low


def z_forward():
    angle = 2 * math.pi * ((np.arange(KZ)[:, None] * np.arange(NZ)[None]) % NZ) / NZ
    high, low = pair(np.concatenate([np.cos(angle), -np.sin(angle)], 0))
    return np.concatenate([high, low], 0)


def y_forward():
    angle = 2 * math.pi * ((waves(KY)[:, None] * np.arange(16)[None]) % NY) / NY
    table = np.zeros((2, 8, 16, 2, KY, 8))
    for x in range(8):
        table[0, x, :, 0, :, x] = np.cos(angle).T
        table[1, x, :, 0, :, x] = np.sin(angle).T
        table[1, x, :, 1, :, x] = np.cos(angle).T
        table[0, x, :, 1, :, x] = -np.sin(angle).T
    high, low = pair(table.reshape(256, 512))
    return np.concatenate([high, low], 0)


def y_phase():
    angle = 2 * math.pi * ((waves(KY)[None] * 16 * np.arange(COLS)[:, None]) % NY) / NY
    scale = 1.0 / (NX * NY * NZ)
    table = np.stack([np.cos(angle), np.sin(angle)], 1) * scale
    return np.repeat(table, 8, axis=2).astype(np.float32)


def x_forward():
    angle = 2 * math.pi * ((waves(KX)[None] * np.arange(8)[:, None]) % NX) / NX
    table = np.zeros((4, 2, 2, 8, 2, 3, 2, 2, KX))
    cosine, sine = np.cos(angle), np.sin(angle)
    for c in range(3):
        for e in range(2):
            for d in range(2):
                table[c, 0, e, :, 0, c, e, d] = cosine
                table[c, 1, e, :, 0, c, e, d] = sine
                table[c, 1, e, :, 1, c, e, d] = cosine
                table[c, 0, e, :, 1, c, e, d] = -sine
    high, low = pair(table.reshape(128, 768))
    return np.concatenate([high, high, low], 0)


def x_phase():
    angle = 2 * math.pi * ((waves(KX)[None] * 8 * np.arange(ROWS)[:, None]) % NX) / NX
    table = np.stack([np.cos(angle), np.sin(angle)], 1)
    return np.tile(table, (1, 1, 4)).astype(np.float32)


def x_inverse():
    points = np.arange(NX).reshape(ROWS, 8)[CHAIN]
    angle = 2 * math.pi * ((points[:, :, None] * waves(KX)) % NX) / NX
    table = np.zeros((ROWS, 2, 8, 2, KX))
    table[:, 0, :, 0] = np.cos(angle)
    table[:, 0, :, 1] = -np.sin(angle)
    table[:, 1, :, 0] = np.sin(angle)
    table[:, 1, :, 1] = np.cos(angle)
    high, low = pair(table.reshape(256, 64))
    return np.concatenate([high, high, low, low], 1)


def y_inverse():
    angle = 2 * math.pi * ((waves(KY)[:, None] * np.arange(NY)[None]) % NY) / NY
    angle = angle.reshape(ROWS, 2, COLS, 16)[CHAIN][:, :, SNAKE].reshape(ROWS, 2, NY).transpose(1, 0, 2)
    table = np.zeros((2, ROWS, 2, 2, NY))
    table[:, :, 0, 0] = np.cos(angle)
    table[:, :, 1, 0] = -np.sin(angle)
    table[:, :, 0, 1] = np.sin(angle)
    table[:, :, 1, 1] = np.cos(angle)
    high, low = pair(table.reshape(64, 512))
    return np.concatenate([high, high, low, low], 0)


def z_inverse():
    angle = 2 * math.pi * ((np.arange(KZ)[:, None] * np.arange(NZ)[None]) % NZ) / NZ
    double = np.where(np.arange(KZ) == 0, 0.5, 1.0)[:, None]
    angle = angle.reshape(COLS, 2, NZ)[SNAKE]
    double = double.reshape(COLS, 2, 1)[SNAKE]
    table = np.stack([double * np.cos(angle), -double * np.sin(angle)], 1)
    high, low = pair(table.reshape(64, NZ))
    return np.concatenate([high, high, low, low], 0)


def dot(a, b):
    return jnp.dot(a, b, preferred_element_type=F32)


def dot_t(a, b):
    return lax.dot_general(a, b, (((1,), (1,)), ((), ())), preferred_element_type=F32)


def split(value):
    high = value.astype(BF16)
    low = (value - high.astype(F32)).astype(BF16)
    return high, low


def exchange(arrays, axis, unit):
    count = len(arrays)
    length = count * unit
    place = lax.broadcasted_iota(jnp.int32, arrays[0].shape, axis)
    arrays = [pltpu.roll(a, m * unit, axis) if m else a for m, a in enumerate(arrays)]
    bit = 1
    while bit < count:
        moved = (place & (bit * unit)) != 0
        arrays = [jnp.where(moved, arrays[(k + bit) % count], arrays[k]) for k in range(count)]
        bit *= 2
    return [arrays[0]] + [pltpu.roll(arrays[count - g], length - g * unit, axis) for g in range(1, count)]


def forward_kernel(step, velocity, tendency, z_table, y_table, phase, advanced, out):
    value = velocity[...] + step[0] * tendency[...]
    advanced[...] = value
    high, low = split(value)
    first = dot_t(z_table[...], high)
    modes = first[:64] + first[64:] + dot_t(z_table[0:64, :], low)
    modes = [
        jnp.concatenate([modes[0:32, 128 * c : 128 * c + 128], modes[32:64, 128 * c : 128 * c + 128]], 1)
        for c in range(3)
    ]
    high, low = split(jnp.concatenate(modes, 0))
    first = dot(jnp.concatenate([high, low], 0), y_table[0:256, :])
    sums = first[:96] + first[96:] + dot(high, y_table[256:512, :])
    turn = phase[lax.axis_index("col")]
    cosine, sine = turn[0:1], turn[1:2]
    parts = []
    for c in range(3):
        re = sums[32 * c : 32 * c + 32, :256]
        im = sums[32 * c : 32 * c + 32, 256:]
        parts.append(re * cosine + im * sine)
        parts.append(im * cosine - re * sine)
    zero = jnp.zeros((32, 128), F32)
    for half in range(2):
        lanes = [p[:, 128 * half : 128 * half + 128] for p in parts] + [zero, zero]
        for g, block in enumerate(exchange(lanes, 1, 16)):
            out[8 * half + g] = block


def prepare_kernel(lift, bias, mixing, mixing_bias, advanced, weights, *rest):
    tables, (w_eff, local), copies = rest[:5], rest[5:7], rest[7:12]
    scratch, lines, held_weights, sems = rest[12:]
    loads = [pltpu.make_async_copy(weights, held_weights, sems.at[0])]
    for k, (source, target) in enumerate(zip(tables, copies)):
        loads.append(pltpu.make_async_copy(source, target, sems.at[1 + k]))
    for load in loads:
        load.start()
    highest = lax.Precision.HIGHEST

    def columns(matrix, vector):
        return lax.dot_general(
            matrix,
            jnp.broadcast_to(vector, (128, 32)),
            (((1,), (1,)), ((), ())),
            precision=highest,
            preferred_element_type=F32,
        )

    local_map = mixing[...]
    eye = jnp.where(
        lax.broadcasted_iota(jnp.int32, (32, 32), 0) == lax.broadcasted_iota(jnp.int32, (32, 32), 1),
        1.0,
        0.0,
    ).astype(F32)
    for j in range(3):
        scratch[j] = 0.5 * columns(local_map, lift[j : j + 1, :])
    scratch[3] = 0.5 * (columns(local_map, bias[...]) + columns(eye, mixing_bias[...]))

    def body(o, carry):
        scale = [scratch[j, pl.ds(o, 1), :] for j in range(4)]
        for half in range(2):
            lanes = slice(128 * half, 128 * half + 128)
            lines[o, :, lanes] = (
                scale[0] * advanced[0:128, lanes]
                + scale[1] * advanced[128:256, lanes]
                + scale[2] * advanced[256:384, lanes]
                + scale[3]
            )
        return carry

    for part in range(4):
        lax.fori_loop(8 * part, 8 * part + 8, body, 0)
        chunk = pl.ds(8 * part, 8)
        loads.append(pltpu.make_async_copy(lines.at[chunk], local.at[chunk], sems.at[6 + part]))
        loads[-1].start()
    row = lax.broadcasted_iota(jnp.int32, (32, 1024), 0)
    lane = lax.broadcasted_iota(jnp.int32, (32, 1024), 1)
    spread = jnp.where(row == (lane & 31), 1.0, 0.0).astype(F32)
    same = row == (lane >> 5)
    maps = []
    for j in range(4):
        source = lift[j : j + 1, :] if j < 3 else bias[...]
        source = jnp.broadcast_to(source, (8, 32))
        wide = jnp.dot(source, spread, precision=highest, preferred_element_type=F32)
        maps.append(jnp.where(same, wide[0:1, :], 0.0))
    maps = jnp.concatenate(maps, 0)
    high, rest = split(maps)
    rest = maps - high.astype(F32)
    mid = rest.astype(BF16)
    low = (rest - mid.astype(F32)).astype(BF16)
    loads[0].wait()
    w = held_weights[...]
    w_eff[...] = dot_t(high, w) + dot_t(mid, w) + dot_t(low, w)
    for load in loads[1:]:
        load.wait()


def mix_kernel(arrived, w_eff, x_table, phase, back_table, out):
    sums = []
    for r in range(ROWS):
        block = arrived[r]
        total = (block[0:8] + block[8:16]) + (block[16:24] + block[24:32])
        total = total + pltpu.roll(total, 4, 0)
        total = total + pltpu.roll(total, 2, 0)
        sums.append(total)
    high, low = split(jnp.concatenate(sums, 0))
    table = x_table[...]
    modes = dot(jnp.concatenate([high, low], 1), table[:256]) + dot(high, table[256:])
    real = [None] * 3
    imag = [None] * 3
    for r in range(ROWS):
        cosine, sine = phase[r, 0:1, :], phase[r, 1:2, :]
        for c in range(3):
            re = modes[8 * r : 8 * r + 8, 128 * c : 128 * c + 128]
            im = modes[8 * r : 8 * r + 8, 384 + 128 * c : 512 + 128 * c]
            a = re * cosine + im * sine
            b = im * cosine - re * sine
            real[c] = a if r == 0 else real[c] + a
            imag[c] = b if r == 0 else imag[c] + b
    row = lax.broadcasted_iota(jnp.int32, (8, 128), 0)
    lane = lax.broadcasted_iota(jnp.int32, (8, 128), 1)
    own = ((lane >> 5) & 1) == (row & 1)

    def spread(value):
        value = jnp.where(own, value, pltpu.roll(value, 1, 0))
        return jnp.concatenate([value] * 4, 0)

    weights = w_eff[...]
    mixed_re = None
    for c in range(3):
        cr, ci = spread(real[c]), spread(imag[c])
        wr = weights[32 * c : 32 * c + 32, :128]
        wi = weights[32 * c : 32 * c + 32, 128:]
        a = wr * cr - wi * ci
        b = wr * ci + wi * cr
        mixed_re = a if c == 0 else mixed_re + a
        mixed_im = b if c == 0 else mixed_im + b
    lane = lax.broadcasted_iota(jnp.int32, (32, 128), 1)
    origin = jnp.logical_and(lane == 0, lax.axis_index("row") + lax.axis_index("col") == 0)
    mixed_re = mixed_re + jnp.where(origin, weights[96:128, :128], 0.0)
    mixed_im = mixed_im + jnp.where(origin, weights[96:128, 128:], 0.0)
    turned = jnp.concatenate([mixed_re, mixed_im, mixed_re, mixed_im], 0).T
    blocks = exchange([turned[32 * k : 32 * k + 32] for k in range(4)], 1, 32)
    high, low = split(jnp.concatenate(blocks[:2], 0))
    stack = jnp.concatenate([high, low, high, low], 0)
    out[...] = dot(back_table[...], stack)


def y_kernel(arrived, table, out):
    parts = []
    for group in range(4):
        tiles = [arrived[64 * group + 8 * k : 64 * group + 8 * k + 8, :] for k in range(8)]
        parts.append(exchange(tiles, 0, 1))
    by_x = [jnp.concatenate([parts[g][x] for g in range(4)], 0) for x in range(8)]
    rows = []
    for two in range(4):
        low_ky, high_ky = exchange([by_x[2 * two], by_x[2 * two + 1]], 1, 64)
        data = jnp.concatenate([low_ky, high_ky], 0)
        high = data.astype(BF16).astype(F32)
        rows.append(jnp.concatenate([high, data - high], 0).T.astype(BF16))
    left = jnp.concatenate(rows, 0)
    left = jnp.concatenate([left, left], 1)
    for part in range(2):
        for half in range(2):
            lane = 256 * part + 128 * half
            cells = dot(left, table[:, lane : lane + 128])
            tiles = [cells[64 * x : 64 * x + 64] for x in range(8)]
            for g, block in enumerate(exchange(tiles, 1, 16)):
                out[8 * half + g, 64 * part : 64 * part + 64, :] = block


def z_kernel(arrived, local, table, out, lines, sems):
    spec = table[...]
    root = math.sqrt(2.0 / math.pi)
    stores = []
    for block in range(4):
        groups = []
        for g in range(8):
            tiles = []
            for k in range(8 * g, 8 * g + 8):
                tiles.append(arrived[k // 4, k % 4, 8 * block : 8 * block + 8, :])
            groups.append(exchange(tiles, 0, 1))
        for o in range(8):
            data = jnp.concatenate([groups[g][o] for g in range(8)], 0)
            high = data.astype(BF16).astype(F32)
            left = jnp.concatenate([high, data - high], 0).T.astype(BF16)
            left = jnp.concatenate([left, left], 1)
            half = dot(left, spec) + local[8 * block + o]
            inner = half * (2.0 * root + (8.0 * root * 0.044715) * (half * half))
            lines[8 * block + o] = (half + half * jnp.tanh(inner)).astype(BF16)
            if o % 4 == 3:
                chunk = pl.ds(8 * block + o - 3, 4)
                k = len(stores)
                stores.append(pltpu.make_async_copy(lines.at[chunk], out.at[chunk], sems.at[k]))
                stores[-1].start()
    for store in stores:
        store.wait()


VMEM = "vmem"
HBM = "hbm"
ANY = "any"
SMEM = "smem"
BLOCKS = {
    VMEM: pl.BlockSpec(memory_space=pltpu.VMEM),
    HBM: pl.BlockSpec(memory_space=pltpu.VMEM),
    ANY: pl.BlockSpec(memory_space=pl.ANY),
    SMEM: pl.BlockSpec(memory_space=pltpu.SMEM),
}


def put(value, where):
    if where == SMEM:
        return value
    space = pltpu.VMEM if where == VMEM else pltpu.HBM
    return pltpu.with_memory_space_constraint(value, space)


def run(kernel, outs, specs, *args, scratch=(), limit=16, out_specs=None):
    return pl.pallas_call(
        kernel,
        out_shape=outs,
        in_specs=[BLOCKS[s] for s in specs],
        out_specs=jax.tree.map(lambda _: BLOCKS[VMEM], outs) if out_specs is None else [BLOCKS[o] for o in out_specs],
        scratch_shapes=scratch,
        compiler_params=pltpu.CompilerParams(vmem_limit_bytes=limit * 1024 * 1024),
        cost_estimate=pl.CostEstimate(flops=1000000, transcendentals=0, bytes_accessed=100000),
    )(*[put(a, s) for a, s in zip(args, specs)])


def per_device(
    velocity, tendency, step_size, lift_weight, lift_bias, spectral_weight, local_weight, local_bias
):
    on_chip = pltpu.VMEM
    advanced, outgoing = run(
        forward_kernel,
        (on_chip((384, 256), F32), on_chip((16, 32, 128), F32)),
        [SMEM] + [HBM] * 5,
        step_size,
        velocity.reshape(384, 256),
        tendency.reshape(384, 256),
        z_forward(),
        y_forward(),
        y_phase(),
    )
    arrived = lax.all_to_all(
        outgoing.reshape(256, 1, 256), ("row", "col"), split_axis=0, concat_axis=0, tiled=True
    ).reshape(16, 32, 128)
    tables = [x_forward(), x_phase(), x_inverse(), y_inverse(), z_inverse()]
    w_eff, local, x_table, turn_table, back_table, y_table, z_table = run(
        prepare_kernel,
        [on_chip((128, 256), F32), pltpu.HBM((32, 128, 256), F32)]
        + [on_chip(t.shape, t.dtype) for t in tables],
        [HBM] * 4 + [VMEM] + [ANY] * 6,
        lift_weight.T,
        lift_bias[None],
        local_weight,
        local_bias[None],
        advanced,
        spectral_weight.reshape(256, 1024),
        *tables,
        scratch=(
            pltpu.VMEM((4, 32, 128), F32),
            pltpu.VMEM((32, 128, 256), F32),
            pltpu.VMEM((256, 1024), BF16),
            pltpu.SemaphoreType.DMA((10,)),
        ),
        out_specs=[VMEM, ANY] + [VMEM] * 5,
    )
    cells_x = run(
        mix_kernel,
        on_chip((256, 128), F32),
        [VMEM] * 5,
        arrived,
        w_eff,
        x_table,
        turn_table,
        back_table,
    )
    by_cells = lax.all_to_all(
        cells_x.reshape(16, 16, 128), "row", split_axis=0, concat_axis=0, tiled=True, axis_index_groups=[CHAIN]
    ).reshape(256, 128)
    cells_y = run(y_kernel, on_chip((16, 128, 128), F32), [VMEM, VMEM], by_cells, y_table)
    pencils = lax.all_to_all(
        cells_y, "col", split_axis=0, concat_axis=0, tiled=True, axis_index_groups=[SNAKE]
    )
    (features,) = run(
        z_kernel,
        [jax.ShapeDtypeStruct((32, 128, 256), BF16)],
        [VMEM] * 3,
        pencils.reshape(16, 4, 32, 128),
        local,
        z_table,
        scratch=(pltpu.VMEM((32, 128, 256), BF16), pltpu.SemaphoreType.DMA((8,))),
        out_specs=[ANY],
    )
    return features.reshape(1, 32, 8, 16, 256)


def solution(mesh):
    in_specs = (
        P(None, None, "row", "col", None),
        P(None, None, "row", "col", None),
        P(),
        P(),
        P(),
        P(None, "row", "col", None, None),
        P(),
        P(),
    )
    out_specs = P(None, None, "row", "col", None)
    return jax.shard_map(
        per_device, mesh=mesh, in_specs=in_specs, out_specs=out_specs, check_vma=False
    )
```
